32 devices in a mesh: parts: 2 (over y), pix: 4 (over z), par: 4 (over x, core).
Axes of the slice: x: 2, y: 2, z: 4, core: 2. Of those that a mesh axis runs over, the one named last changes fastest.
Arguments:
- green_matrix: bfloat16 [4608, 16384], P('pix', 'par'), may hold values from -0.046875 to 0.046875
- observed: bfloat16 [64, 4608], P('parts', 'pix'), parts along dimension 0, may hold values from -1000 to 1000
Outputs:
- solution: float32 [64, 16384], P('parts', 'par'), parts along dimension 0
- residual: float32 [64, 4608], P('parts', 'pix'), parts along dimension 0
The draws below stay inside these ranges and needn't reach their ends.
There are 2 independent parts, one for each index of `parts`. The reference program is written for one: setup_inputs(seed, part) draws one part's arguments, and reference() takes and returns one part's arrays. A program takes and returns all parts, laid end to end along the dimension named above; an argument that names none is the same for every part. Nothing has to cross between parts.
All inputs are finite; a program needn't handle non-finite values.
Results may differ from the reference program's by a relative error of at most 0.0038.
Values may be sent and summed in bfloat16 or wider, within the bound.
A program may use at most 64 MiB of HBM per device.

```python
import math
import jax
import jax.numpy as jnp
from jax import lax

GRID = 128
PARAMS = 16384
SETS = 32
PIXELS = 4608
ITERS = 5


def draw_green_matrix(key, part):
    keys = jax.random.split(jax.random.fold_in(key, 29), 4)
    base = jnp.clip(jax.random.normal(keys[0], (PIXELS, PARAMS), jnp.float32), -6.0, 6.0)
    column_scale = jnp.exp(jax.random.uniform(keys[1], (1, PARAMS), jnp.float32, -2.5, 0.0))
    left = jax.random.normal(keys[2], (PIXELS, 3), jnp.float32)
    right = jax.random.normal(keys[3], (3, PARAMS), jnp.float32)
    common = left[:, 0:1] * right[0:1, :] + left[:, 1:2] * right[1:2, :] + left[:, 2:3] * right[2:3, :]
    common = common / math.sqrt(3.0)
    place = jnp.arange(PARAMS, dtype=jnp.float32)[None, :] / PARAMS - 1.0
    rising = jnp.exp(math.log(3.0) * place)
    value = (base + 0.06 * common) * column_scale * rising * (2.2 / GRID)
    bound = 6.0 / GRID
    return jnp.clip(value, -bound, bound).astype(jnp.bfloat16)


def draw_observed(key, part):
    keys = jax.random.split(jax.random.fold_in(key, 71), 3)
    position = jnp.arange(PIXELS, dtype=jnp.float32) / PIXELS
    base = jnp.clip(jax.random.normal(keys[0], (SETS, PIXELS), jnp.float32), -6.0, 6.0)
    rising = jnp.exp(math.log(3.0) * position)[None, :]
    row_scale = jnp.exp(jax.random.uniform(keys[1], (1, PIXELS), jnp.float32, math.log(0.5), math.log(5.0)))
    set_scale = jnp.exp(jax.random.uniform(keys[2], (SETS, 1), jnp.float32, math.log(0.3), math.log(3.0)))
    return (base * rising * row_scale * set_scale).astype(jnp.bfloat16)


def setup_inputs(seed: int = 0, part: int = 0) -> dict:
    seeds = jax.random.split(jax.random.key(seed), 3)
    own_keys = jax.random.split(jax.random.fold_in(seeds[2], part), 3)
    green_matrix = draw_green_matrix(jax.random.fold_in(seeds[2], 71), part)
    observed = draw_observed(jax.random.fold_in(jax.random.fold_in(seeds[2], part), 71), part)
    return {"green_matrix": green_matrix, "observed": observed}


def smooth(values):
    set_count = values.shape[0]
    tiles = values.reshape(set_count, GRID, GRID)
    padded = jnp.pad(tiles, ((0, 0), (1, 1), (1, 1)))
    beside_all = padded[:, 2:, 1:-1] + padded[:, :-2, 1:-1] + padded[:, 1:-1, 2:] + padded[:, 1:-1, :-2]
    return (0.25 * (4.0 * tiles - beside_all)).reshape(set_count, GRID * GRID)


def reference(green_matrix, observed):
    residual = observed.astype(jnp.float32)
    gradient = jnp.dot(observed, green_matrix, preferred_element_type=jnp.float32)
    grad_sq = jnp.sum(gradient * gradient, axis=1)
    direction = gradient
    solution = jnp.zeros((SETS, GRID * GRID), jnp.float32)
    smooth_res = jnp.zeros((SETS, GRID * GRID), jnp.float32)
    for sweep in range(ITERS):
        rounded = direction.astype(jnp.bfloat16)
        image = lax.dot_general(rounded, green_matrix, (((1,), (1,)), ((), ())), preferred_element_type=jnp.float32)
        smoothed = smooth(lax.optimization_barrier(rounded).astype(jnp.float32))
        curvature = jnp.sum(image * image, axis=1) + jnp.sum(smoothed * smoothed, axis=1)
        step_len = (grad_sq / curvature)[:, None]
        solution = solution + step_len * direction
        residual = residual - step_len * image
        smooth_res = smooth_res - step_len * smoothed
        if sweep + 1 < ITERS:
            gradient = jnp.dot(residual.astype(jnp.bfloat16), green_matrix, preferred_element_type=jnp.float32) + smooth(smooth_res)
            fresh_sq = jnp.sum(gradient * gradient, axis=1)
            direction = gradient + (fresh_sq / grad_sq)[:, None] * direction
            grad_sq = fresh_sq
    return solution, residual
```

```python
import functools

import jax
import jax.numpy as jnp
from jax import lax
from jax.experimental import pallas as pl
from jax.experimental.pallas import tpu as pltpu
from jax.sharding import PartitionSpec as P

GRID = 128
ITERS = 5
LANES = 128
SUB = 2
GROUPS = 2
RELAYS = {}


def padded_2(block, sides, width):
    for axis, dim in sides:
        count = lax.axis_size(axis)
        forward = [(i, i + 1) for i in range(count - 1)]
        backward = [(target, source) for source, target in forward]
        low = lax.ppermute(
            lax.slice_in_dim(block, block.shape[dim] - width, None, axis=dim), axis, forward
        )
        high = lax.ppermute(lax.slice_in_dim(block, 0, width, axis=dim), axis, backward)
        block = jnp.concatenate([low, block, high], axis=dim)
    return block


def smooth(values):
    set_count = values.shape[0]
    grid_rows = values.shape[1] // GRID
    tiles = values.reshape(set_count, grid_rows, GRID)
    padded = padded_2(tiles, (("par", 1),), 1)
    padded = jnp.pad(padded, ((0, 0), (0, 0), (1, 1)))
    beside_all = (
        padded[:, 2:, 1:-1] + padded[:, :-2, 1:-1] + padded[:, 1:-1, 2:] + padded[:, 1:-1, :-2]
    )
    return (0.25 * (4.0 * tiles - beside_all)).reshape(set_count, grid_rows * GRID)


def forward(rounded, green_matrix):
    partial_value = lax.dot_general(
        rounded, green_matrix, (((1,), (1,)), ((), ())), preferred_element_type=jnp.float32
    )
    return lax.psum(partial_value, "par")


def curvatures(image, smoothed):
    local_image = jnp.sum(image * image, axis=1)
    local_smooth = jnp.sum(smoothed * smoothed, axis=1)
    image_sq = lax.psum(local_image, "pix")
    smooth_sq = lax.psum(local_smooth, "par")
    return image_sq + smooth_sq


def backward_sum(rounded, green_matrix):
    return lax.psum(jnp.dot(rounded, green_matrix, preferred_element_type=jnp.float32), "pix")


def column_squares(gradient):
    return lax.psum(jnp.sum(gradient * gradient, axis=1), "par")


def on_device(green_matrix, observed):
    set_count = observed.shape[0]
    tile_cells = green_matrix.shape[1]
    residual = observed.astype(jnp.float32)
    gradient = backward_sum(observed, green_matrix)
    grad_sq = column_squares(gradient)
    direction = gradient
    solution = jnp.zeros((set_count, tile_cells), jnp.float32)
    smooth_res = jnp.zeros((set_count, tile_cells), jnp.float32)
    for sweep in range(ITERS):
        rounded = direction.astype(jnp.bfloat16)
        image = forward(rounded, green_matrix)
        smoothed = smooth(lax.optimization_barrier(rounded).astype(jnp.float32))
        step_len = (grad_sq / curvatures(image, smoothed))[:, None]
        solution = solution + step_len * direction
        residual = residual - step_len * image
        smooth_res = smooth_res - step_len * smoothed
        if sweep + 1 < ITERS:
            gradient = backward_sum(residual.astype(jnp.bfloat16), green_matrix) + smooth(
                smooth_res
            )
            fresh_sq = column_squares(gradient)
            direction = gradient + (fresh_sq / grad_sq)[:, None] * direction
            grad_sq = fresh_sq
    return (solution, residual)


MESH = pl.DeviceIdType.MESH


def to_row(column):
    count = column.shape[0]
    eye = lax.broadcasted_iota(jnp.int32, (count, LANES), 0) == lax.broadcasted_iota(
        jnp.int32, (count, LANES), 1
    )
    return jnp.sum(jnp.where(eye, jnp.broadcast_to(column, (count, LANES)), 0.0), axis=0, keepdims=True)


def to_column(row, count):
    eye = lax.broadcasted_iota(jnp.int32, (count, LANES), 0) == lax.broadcasted_iota(
        jnp.int32, (count, LANES), 1
    )
    return jnp.sum(jnp.where(eye, jnp.broadcast_to(row, (count, LANES)), 0.0), axis=1, keepdims=True)


def flipped(index, mask, count):
    value, bit = 0, 1
    while bit < count:
        digit = lax.rem(index // bit, 2)
        value = value + bit * (1 - digit if mask & bit else digit)
        bit *= 2
    return value


def far_first(count):
    masks = []
    bit = count // 2
    while bit:
        masks += range(bit, 2 * bit)
        bit //= 2
    return masks


def stencil(above, here, below):
    lane = lax.broadcasted_iota(jnp.int32, here.shape, 1)
    left = jnp.where(lane == 0, 0.0, pltpu.roll(here, 1, 1))
    right = jnp.where(lane == GRID - 1, 0.0, pltpu.roll(here, GRID - 1, 1))
    return here - 0.25 * (above + below + left + right)


def cgls_kernel(
    nz, npar,
    green_hbm, obs_ref, x_ref, r_ref,
    green, imb, im, own_image, p_ext, sp, g_own, own_part, gg_ref,
    rs_send, rs_recv, ag, h_recv, halo,
    sz, sp_scalar, nz_scalar, npar_scalar,
    load_sem, rs_ss, rs_rs, ag_ss, ag_rs, relay_ss, h_ss, h_rs, halo_ss, halo_rs,
    sz_ss, sz_rs, sp_ss, sp_rs, nz_ss, nz_rs, np_ss, np_rs,
):
    me_z = lax.axis_index("pix")
    me_p = lax.axis_index("par")
    core = lax.rem(me_p, 2)
    chip = me_p // 2
    nchip = npar // 2
    partner = me_p + 1 - 2 * core
    size = obs_ref.shape[0] // GROUPS
    groups = range(GROUPS)
    width = green.shape[3]
    rows = nz * SUB * width // GRID
    own_rows = width // GRID
    edge = 2 * GRID
    z_peers = [flipped(me_z, mask, nz) for mask in far_first(nz)]
    z_from = z_peers[::-1]
    p_peers = [
        2 * lax.rem(chip + i, nchip) + c for i in range(1, nchip) for c in range(2)
    ] + [partner]
    order = [(s, c) for s in range(SUB) for c in z_peers] + [(s, me_z) for s in range(SUB)]

    def load(s, c):
        first = pl.multiple_of((c * SUB + s) * width, width)
        return pltpu.make_async_copy(
            green_hbm.at[:, pl.ds(first, width)], green.at[c, s], load_sem.at[c, s]
        )

    for s, c in order:
        load(s, c).start()

    barrier = pltpu.get_barrier_semaphore()
    for j in range(1, nz):
        pl.semaphore_signal(barrier, inc=1, device_id={"pix": lax.rem(me_z + j, nz)}, device_id_type=MESH)
    for j in range(1, npar):
        pl.semaphore_signal(barrier, inc=1, device_id={"par": lax.rem(me_p + j, npar)}, device_id_type=MESH)

    for g in groups:
        mine = slice(g * size, (g + 1) * size)
        imb[g] = obs_ref[mine]
        r_ref[mine] = obs_ref[mine].astype(jnp.float32)
    im[...] = jnp.zeros_like(im)
    p_ext[...] = jnp.zeros_like(p_ext)
    sp[...] = jnp.zeros_like(sp)
    sz[0] = jnp.zeros_like(sz[0])
    sp_scalar[0] = jnp.zeros_like(sp_scalar[0])
    g_own[...] = jnp.zeros_like(g_own)
    gg_ref[...] = jnp.zeros_like(gg_ref)
    x_ref[...] = jnp.zeros_like(x_ref)

    with jax.named_scope("barrier"):
        pl.semaphore_wait(barrier, nz + npar - 2)

    def z_copy(buf, ssem, rsem, k, g, source, target, *s):
        return pltpu.make_async_remote_copy(
            src_ref=buf.at[(k, g, source, *s)], dst_ref=buf.at[(k, g, source, *s)],
            send_sem=ssem.at[(k, g, target, *s)], recv_sem=rsem.at[(k, g, source, *s)],
            device_id={"pix": target}, device_id_type=MESH,
        )

    def to_z(buf, ssem, rsem, k, g, peer, *s):
        return z_copy(buf, ssem, rsem, k, g, me_z, peer, *s)

    def from_z(buf, ssem, rsem, k, g, peer, *s):
        return z_copy(buf, ssem, rsem, k, g, peer, peer, *s)

    def par_copy(buf, ssem, rsem, k, g, source, target):
        return pltpu.make_async_remote_copy(
            src_ref=buf.at[k, g, source], dst_ref=buf.at[k, g, source],
            send_sem=ssem.at[k, g, target], recv_sem=rsem.at[k, g, source],
            device_id={"par": target}, device_id_type=MESH,
        )

    def to_par(buf, ssem, rsem, k, g, peer):
        return par_copy(buf, ssem, rsem, k, g, me_p, peer)

    def from_par(buf, ssem, rsem, k, g, peer):
        return par_copy(buf, ssem, rsem, k, g, peer, peer)

    image_sq = (sz, sz_ss, sz_rs)
    smooth_sq = (sp_scalar, sp_ss, sp_rs)
    pix_sq = (nz_scalar, nz_ss, nz_rs)
    par_sq = (npar_scalar, np_ss, np_rs)
    gathered = (ag, ag_ss, ag_rs)
    images = (h_recv, h_ss, h_rs)

    def total_row(parts):
        value = parts[0]
        for part in parts[1:]:
            value = value + part
        return value

    def z_row(buf, k, g):
        return total_row([buf[k, g, i, 0:1] for i in range(nz)])

    def par_row(buf, k, g):
        return total_row([buf[k, g, i, 0:1] for i in range(npar)])

    def send_image_sq(k, g):
        image = im[g]
        row = to_row(jnp.sum(image * image, axis=1, keepdims=True))
        sz[k, g, me_z] = jnp.broadcast_to(row, (8, LANES))
        for peer in z_peers:
            to_z(*image_sq, k, g, peer).start()

    def send_smooth_sq(k, g):
        square = jnp.zeros((size, GRID), jnp.float32)
        for i in range(rows + 2):
            line = stencil(
                p_ext[g, :, i * GRID:(i + 1) * GRID],
                p_ext[g, :, (i + 1) * GRID:(i + 2) * GRID],
                p_ext[g, :, (i + 2) * GRID:(i + 3) * GRID],
            )
            if i == 0:
                line = jnp.where(me_p == 0, 0.0, line)
            elif i == rows + 1:
                line = jnp.where(me_p == npar - 1, 0.0, line)
            else:
                square = square + line * line
            sp[g, :, i * GRID:(i + 1) * GRID] = line
        row = to_row(jnp.sum(square, axis=1, keepdims=True))
        sp_scalar[k, g, me_p] = jnp.broadcast_to(row, (8, LANES))
        for peer in p_peers:
            to_par(*smooth_sq, k, g, peer).start()

    def wait_curvature(k, g):
        for peer in p_peers:
            from_par(*smooth_sq, k, g, peer).wait_recv()
        for peer in z_from:
            from_z(*image_sq, k, g, peer).wait_recv()

    def step_row(k, g):
        return gg_ref[g, 0:1] / (z_row(sz, k, g) + par_row(sp_scalar, k, g))

    def apply_step(step, g):
        mine = slice(g * size, (g + 1) * size)
        x_ref[mine] += step * p_ext[g, :, edge:edge + rows * GRID]
        r_ref[mine] -= step * im[g]

    def finish_curvature(k, g):
        for peer in z_peers:
            to_z(*image_sq, k, g, peer).wait_send()
        for peer in p_peers:
            to_par(*smooth_sq, k, g, peer).wait_send()

    def rs_copy(k, g, target, s):
        return pltpu.make_async_remote_copy(
            src_ref=rs_send.at[k, g, target, s], dst_ref=rs_recv.at[k, g, me_z, s],
            send_sem=rs_ss.at[k, g, target, s], recv_sem=rs_rs.at[k, g, me_z, s],
            device_id={"pix": target}, device_id_type=MESH,
        )

    def rs_from(k, g, source, s):
        return pltpu.make_async_remote_copy(
            src_ref=rs_send.at[k, g, source, s], dst_ref=rs_recv.at[k, g, source, s],
            send_sem=rs_ss.at[k, g, source, s], recv_sem=rs_rs.at[k, g, source, s],
            device_id={"pix": source}, device_id_type=MESH,
        )

    def relayed(g, s):
        return (g, s) in RELAYS

    def sent_to(g, s):
        return [flipped(me_z, mask, nz) for mask in far_first(nz) if not relayed(g, s) or mask != 3]

    def relay_copy(k, g, s):
        cross = flipped(me_z, 2, nz)
        return z_copy(ag, relay_ss, ag_rs, k, g, cross, flipped(me_z, 1, nz), s)

    def relays(k, point):
        for (g, s), place in RELAYS.items():
            if place == point:
                with jax.named_scope("relay%d" % g):
                    from_z(*gathered, k, g, flipped(me_z, 2, nz), s).wait_recv()
                    relay_copy(k, g, s).start()

    up = lax.rem(me_p + 1, npar)
    down = lax.rem(me_p + npar - 1, npar)

    def halo_copies(k, g):
        return (
            pltpu.make_async_remote_copy(
                src_ref=ag.at[k, g, nz - 1, SUB - 1, :, pl.ds(width - edge, edge)],
                dst_ref=halo.at[k, g, 0],
                send_sem=halo_ss.at[k, g, 0], recv_sem=halo_rs.at[k, g, 0],
                device_id={"par": up}, device_id_type=MESH,
            ),
            pltpu.make_async_remote_copy(
                src_ref=ag.at[k, g, 0, 0, :, pl.ds(0, edge)],
                dst_ref=halo.at[k, g, 1],
                send_sem=halo_ss.at[k, g, 1], recv_sem=halo_rs.at[k, g, 1],
                device_id={"par": down}, device_id_type=MESH,
            ),
        )

    def scatter(k, g):
        vector = imb[g]

        def backward(s, c):
            if g == 0:
                @pl.when(k == 0)
                def _():
                    load(s, c).wait()

            return jnp.dot(vector, green[c, s], preferred_element_type=jnp.float32)

        with jax.named_scope("bwd%d" % g):
            for s in range(SUB):
                for peer in z_peers:
                    rs_send[k, g, peer, s] = backward(s, peer).astype(jnp.bfloat16)
                    rs_copy(k, g, peer, s).start()
        with jax.named_scope("own%d" % g):
            for s in range(SUB):
                base = (me_z * SUB + s) * own_rows
                lines = []
                for i in range(own_rows):
                    lines.append(stencil(*[
                        sp[g, :, pl.ds(pl.multiple_of((base + i + d) * GRID, GRID), GRID)]
                        for d in range(3)
                    ]))
                own_part[g, s] = backward(s, me_z) + jnp.concatenate(lines, axis=1)

    def gather(k, g):
        with jax.named_scope("curv%d" % g):
            @pl.when(k > 0)
            def _():
                wait_curvature(k, g)

            step = to_column(jnp.where(k == 0, -1.0, step_row(k, g)), size)
        square = jnp.zeros((size, 1), jnp.float32)
        for s in range(SUB):
            with jax.named_scope("rs%d" % g):
                for source in z_from:
                    rs_from(k, g, source, s).wait_recv()
            with jax.named_scope("upd%d" % g):
                fresh = own_part[g, s]
                for source in z_from:
                    fresh = fresh + rs_recv[k, g, source, s].astype(jnp.float32)
                gradient = g_own[g, s] - step * fresh
                g_own[g, s] = gradient
                ag[k, g, me_z, s] = gradient.astype(jnp.bfloat16)
                for peer in sent_to(g, s):
                    to_z(*gathered, k, g, peer, s).start()
                square = square + jnp.sum(gradient * gradient, axis=1, keepdims=True)
            relays(k, "g%d%d" % (g, s))
        with jax.named_scope("app%d" % g):
            nz_scalar[k, g, me_z] = jnp.broadcast_to(to_row(square), (8, LANES))
            for peer in z_peers:
                to_z(*pix_sq, k, g, peer).start()
            apply_step(step, g)

    def forward(k, g, s, c):
        return lax.dot_general(
            ag[k, g, c, s], green[c, s], (((1,), (1,)), ((), ())),
            preferred_element_type=jnp.float32,
        )

    def forward_own(k, g):
        with jax.named_scope("fown%d" % g):
            image = forward(k, g, 0, me_z)
            for s in range(1, SUB):
                image = image + forward(k, g, s, me_z)
            own_image[g] = image

    def forward_rest(k, g):
        image = own_image[g]
        with jax.named_scope("frest%d" % g):
            seq = [(s, mask) for s in range(SUB) for mask in ((1, 2) if relayed(g, s) else (1, 3, 2))]
            late = [(s, 3) for s in range(SUB) if relayed(g, s)]
            cut = len(seq) - 3
            seq = seq[:cut] + late[:1] + seq[cut:] + late[1:]
            for i, (s, mask) in enumerate(seq):
                source = flipped(me_z, mask, nz)
                if not (relayed(g, s) and mask == 2):
                    from_z(*gathered, k, g, source, s).wait_recv()
                if i + 1 == len(seq):
                    for copy in halo_copies(k, g):
                        copy.start()
                image = image + forward(k, g, s, source)
                relays(k, "f%d%d" % (g, i))
                if i == 2:
                    for source in z_from:
                        from_z(*pix_sq, k, g, source).wait_recv()
                    npar_scalar[k, g, me_p] = jnp.broadcast_to(z_row(nz_scalar, k, g), (8, LANES))
                    for peer in p_peers:
                        to_par(*par_sq, k, g, peer).start()
        with jax.named_scope("hsend%d" % g):
            h_recv[k, g, me_p] = image.astype(jnp.bfloat16)
            for peer in p_peers:
                to_par(*images, k, g, peer).start()

    def advance(k, g):
        with jax.named_scope("npw%d" % g):
            for peer in p_peers:
                from_par(*par_sq, k, g, peer).wait_recv()
            for copy in halo_copies(k, g):
                copy.wait_recv()
        with jax.named_scope("pupd%d" % g):
            fresh_sq = par_row(npar_scalar, k, g)
            ratio = to_column(jnp.where(k == 0, 0.0, fresh_sq / gg_ref[g, 0:1]), size)
            gg_ref[g] = jnp.broadcast_to(fresh_sq, (8, LANES))
            for c in range(nz):
                for s in range(SUB):
                    first = edge + (c * SUB + s) * width
                    where = slice(first, first + width)
                    p_ext[g, :, where] = (
                        ag[k, g, c, s].astype(jnp.float32) + ratio * p_ext[g, :, where]
                    )
            first = jnp.where(me_p == 0, 0.0, halo[k, g, 0].astype(jnp.float32))
            p_ext[g, :, :edge] = first + ratio * p_ext[g, :, :edge]
            last = jnp.where(me_p == npar - 1, 0.0, halo[k, g, 1].astype(jnp.float32))
            p_ext[g, :, edge + rows * GRID:] = last + ratio * p_ext[g, :, edge + rows * GRID:]
            send_smooth_sq(k + 1, g)
        with jax.named_scope("hw%d" % g):
            for peer in p_peers:
                from_par(*images, k, g, peer).wait_recv()
        with jax.named_scope("im%d" % g):
            part = h_recv[k, g, 0].astype(jnp.float32)
            for i in range(1, npar):
                part = part + h_recv[k, g, i].astype(jnp.float32)
            image = part + ratio * im[g]
            im[g] = image
            imb[g] = image.astype(jnp.bfloat16)
            send_image_sq(k + 1, g)

    def finish_sends(k, g):
        for peer in z_peers:
            for s in range(SUB):
                rs_copy(k, g, peer, s).wait_send()
            to_z(*pix_sq, k, g, peer).wait_send()
        for s in range(SUB):
            for peer in sent_to(g, s):
                to_z(*gathered, k, g, peer, s).wait_send()
            if relayed(g, s):
                relay_copy(k, g, s).wait_send()
        for copy in halo_copies(k, g):
            copy.wait_send()
        for peer in p_peers:
            to_par(*par_sq, k, g, peer).wait_send()
            to_par(*images, k, g, peer).wait_send()
        finish_curvature(k + 1, g)

    @pl.loop(0, ITERS)
    def _(k):
        @pl.when(k > 0)
        def _():
            advance(k - 1, 0)

        scatter(k, 0)

        @pl.when(k > 0)
        def _():
            forward_rest(k - 1, 1)
            finish_sends(k - 1, 0)

        gather(k, 0)
        forward_own(k, 0)

        @pl.when(k > 0)
        def _():
            advance(k - 1, 1)

        scatter(k, 1)

        @pl.when(k > 0)
        def _():
            finish_sends(k - 1, 1)

        forward_rest(k, 0)
        gather(k, 1)
        forward_own(k, 1)

    advance(ITERS - 1, 0)
    forward_rest(ITERS - 1, 1)
    with jax.named_scope("final"):
        finish_sends(ITERS - 1, 0)
        wait_curvature(ITERS, 0)
        apply_step(to_column(step_row(ITERS, 0), size), 0)
    advance(ITERS - 1, 1)
    with jax.named_scope("final2"):
        finish_sends(ITERS - 1, 1)
        wait_curvature(ITERS, 1)
        apply_step(to_column(step_row(ITERS, 1), size), 1)


def finish_kernel(x_ref, r_ref, x_out, r_out, x_sem, r_sem):
    copies = (
        pltpu.make_async_copy(x_ref, x_out, x_sem),
        pltpu.make_async_copy(r_ref, r_out, r_sem),
    )
    for copy in copies:
        copy.start()
    for copy in copies:
        copy.wait()


def finish(x, r):
    vmem = pl.BlockSpec(memory_space=pltpu.VMEM)
    space = pl.BlockSpec(memory_space=pl.ANY)
    return pl.pallas_call(
        finish_kernel,
        out_shape=(jax.ShapeDtypeStruct(x.shape, x.dtype), jax.ShapeDtypeStruct(r.shape, r.dtype)),
        in_specs=[vmem, vmem],
        out_specs=(space, space),
        scratch_shapes=[pltpu.SemaphoreType.DMA, pltpu.SemaphoreType.DMA],
    )(x, r)


def on_device_kernel(nz, npar, green_matrix, observed):
    sets, pixels = observed.shape
    cells = green_matrix.shape[1]
    width = cells // (nz * SUB)
    size = sets // GROUPS
    bf16, f32 = jnp.bfloat16, jnp.float32
    dma = pltpu.SemaphoreType.DMA
    n = ITERS
    vmem = pl.BlockSpec(memory_space=pltpu.VMEM)
    return pl.pallas_call(
        functools.partial(cgls_kernel, nz, npar),
        out_shape=(
            jax.ShapeDtypeStruct((sets, cells), f32),
            jax.ShapeDtypeStruct((sets, pixels), f32),
        ),
        in_specs=[pl.BlockSpec(memory_space=pl.ANY), vmem],
        out_specs=(vmem, vmem),
        scratch_shapes=[
            pltpu.VMEM((nz, SUB, pixels, width), bf16),
            pltpu.VMEM((GROUPS, size, pixels), bf16),
            pltpu.VMEM((GROUPS, size, pixels), f32),
            pltpu.VMEM((GROUPS, size, pixels), f32),
            pltpu.VMEM((GROUPS, size, cells + 4 * GRID), f32),
            pltpu.VMEM((GROUPS, size, cells + 2 * GRID), f32),
            pltpu.VMEM((GROUPS, SUB, size, width), f32),
            pltpu.VMEM((GROUPS, SUB, size, width), f32),
            pltpu.VMEM((GROUPS, 8, LANES), f32),
            pltpu.VMEM((n, GROUPS, nz, SUB, size, width), bf16),
            pltpu.VMEM((n, GROUPS, nz, SUB, size, width), bf16),
            pltpu.VMEM((n, GROUPS, nz, SUB, size, width), bf16),
            pltpu.VMEM((n, GROUPS, npar, size, pixels), bf16),
            pltpu.VMEM((n, GROUPS, 2, size, 2 * GRID), bf16),
            pltpu.VMEM((n + 1, GROUPS, nz, 8, LANES), f32),
            pltpu.VMEM((n + 1, GROUPS, npar, 8, LANES), f32),
            pltpu.VMEM((n, GROUPS, nz, 8, LANES), f32),
            pltpu.VMEM((n, GROUPS, npar, 8, LANES), f32),
            dma((nz, SUB)),
            dma((n, GROUPS, nz, SUB)), dma((n, GROUPS, nz, SUB)),
            dma((n, GROUPS, nz, SUB)), dma((n, GROUPS, nz, SUB)),
            dma((n, GROUPS, nz, SUB)),
            dma((n, GROUPS, npar)), dma((n, GROUPS, npar)),
            dma((n, GROUPS, 2)), dma((n, GROUPS, 2)),
            dma((n + 1, GROUPS, nz)), dma((n + 1, GROUPS, nz)),
            dma((n + 1, GROUPS, npar)), dma((n + 1, GROUPS, npar)),
            dma((n, GROUPS, nz)), dma((n, GROUPS, nz)),
            dma((n, GROUPS, npar)), dma((n, GROUPS, npar)),
        ],
        compiler_params=pltpu.CompilerParams(
            collective_id=0, has_side_effects=True, vmem_limit_bytes=60 * 1024 * 1024
        ),
    )(green_matrix, observed)


def solution(mesh):
    nz, npar = mesh.shape["pix"], mesh.shape["par"]

    def step(green_matrix, observed):
        sets, cells = observed.shape[0], green_matrix.shape[1]
        width = cells // (nz * SUB)
        fits = cells % (nz * SUB * GRID) == 0 and width >= 2 * GRID and nz & (nz - 1) == 0
        if fits and nz > 1 and npar % 2 == 0 and sets % 32 == 0 and sets <= LANES:
            return finish(*on_device_kernel(nz, npar, green_matrix, observed))
        return on_device(green_matrix, observed)

    return jax.shard_map(
        step,
        mesh=mesh,
        in_specs=(P("pix", "par"), P("parts", "pix")),
        out_specs=(P("parts", "par"), P("parts", "pix")),
        check_vma=False,
    )
```

```python
import functools

import jax
import jax.numpy as jnp
from jax import lax
from jax.experimental import pallas as pl
from jax.experimental.pallas import tpu as pltpu
from jax.sharding import PartitionSpec as P

GRID = 128
ITERS = 5
LANES = 128
SUB = 2
GROUPS = 2


def padded_2(block, sides, width):
    for axis, dim in sides:
        count = lax.axis_size(axis)
        forward = [(i, i + 1) for i in range(count - 1)]
        backward = [(target, source) for source, target in forward]
        low = lax.ppermute(
            lax.slice_in_dim(block, block.shape[dim] - width, None, axis=dim), axis, forward
        )
        high = lax.ppermute(lax.slice_in_dim(block, 0, width, axis=dim), axis, backward)
        block = jnp.concatenate([low, block, high], axis=dim)
    return block


def smooth(values):
    set_count = values.shape[0]
    grid_rows = values.shape[1] // GRID
    tiles = values.reshape(set_count, grid_rows, GRID)
    padded = padded_2(tiles, (("par", 1),), 1)
    padded = jnp.pad(padded, ((0, 0), (0, 0), (1, 1)))
    beside_all = (
        padded[:, 2:, 1:-1] + padded[:, :-2, 1:-1] + padded[:, 1:-1, 2:] + padded[:, 1:-1, :-2]
    )
    return (0.25 * (4.0 * tiles - beside_all)).reshape(set_count, grid_rows * GRID)


def forward(rounded, green_matrix):
    partial_value = lax.dot_general(
        rounded, green_matrix, (((1,), (1,)), ((), ())), preferred_element_type=jnp.float32
    )
    return lax.psum(partial_value, "par")


def curvatures(image, smoothed):
    local_image = jnp.sum(image * image, axis=1)
    local_smooth = jnp.sum(smoothed * smoothed, axis=1)
    image_sq = lax.psum(local_image, "pix")
    smooth_sq = lax.psum(local_smooth, "par")
    return image_sq + smooth_sq


def backward_sum(rounded, green_matrix):
    return lax.psum(jnp.dot(rounded, green_matrix, preferred_element_type=jnp.float32), "pix")


def column_squares(gradient):
    return lax.psum(jnp.sum(gradient * gradient, axis=1), "par")


def on_device(green_matrix, observed):
    set_count = observed.shape[0]
    tile_cells = green_matrix.shape[1]
    residual = observed.astype(jnp.float32)
    gradient = backward_sum(observed, green_matrix)
    grad_sq = column_squares(gradient)
    direction = gradient
    solution = jnp.zeros((set_count, tile_cells), jnp.float32)
    smooth_res = jnp.zeros((set_count, tile_cells), jnp.float32)
    for sweep in range(ITERS):
        rounded = direction.astype(jnp.bfloat16)
        image = forward(rounded, green_matrix)
        smoothed = smooth(lax.optimization_barrier(rounded).astype(jnp.float32))
        step_len = (grad_sq / curvatures(image, smoothed))[:, None]
        solution = solution + step_len * direction
        residual = residual - step_len * image
        smooth_res = smooth_res - step_len * smoothed
        if sweep + 1 < ITERS:
            gradient = backward_sum(residual.astype(jnp.bfloat16), green_matrix) + smooth(
                smooth_res
            )
            fresh_sq = column_squares(gradient)
            direction = gradient + (fresh_sq / grad_sq)[:, None] * direction
            grad_sq = fresh_sq
    return (solution, residual)


MESH = pl.DeviceIdType.MESH


def to_row(column):
    count = column.shape[0]
    eye = lax.broadcasted_iota(jnp.int32, (count, LANES), 0) == lax.broadcasted_iota(
        jnp.int32, (count, LANES), 1
    )
    return jnp.sum(jnp.where(eye, jnp.broadcast_to(column, (count, LANES)), 0.0), axis=0, keepdims=True)


def to_column(row, count):
    eye = lax.broadcasted_iota(jnp.int32, (count, LANES), 0) == lax.broadcasted_iota(
        jnp.int32, (count, LANES), 1
    )
    return jnp.sum(jnp.where(eye, jnp.broadcast_to(row, (count, LANES)), 0.0), axis=1, keepdims=True)


def flipped(index, mask, count):
    value, bit = 0, 1
    while bit < count:
        digit = lax.rem(index // bit, 2)
        value = value + bit * (1 - digit if mask & bit else digit)
        bit *= 2
    return value


def far_first(count):
    masks = []
    bit = count // 2
    while bit:
        masks += range(2 * bit - 1, bit - 1, -1)
        bit //= 2
    return masks


def stencil(above, here, below):
    lane = lax.broadcasted_iota(jnp.int32, here.shape, 1)
    left = jnp.where(lane == 0, 0.0, pltpu.roll(here, 1, 1))
    right = jnp.where(lane == GRID - 1, 0.0, pltpu.roll(here, GRID - 1, 1))
    return here - 0.25 * (above + below + left + right)


def cgls_kernel(
    nz, npar,
    green_hbm, obs_ref, x_ref, r_ref,
    green, green_t, imb, im, own_image, p_ext, sp, g_own, own_part, gg_ref,
    rs_send, rs_recv, ag, h_recv, halo,
    sz, sp_scalar, nz_scalar, npar_scalar,
    load_sem, rs_ss, rs_rs, ag_ss, ag_rs, h_ss, h_rs, halo_ss, halo_rs,
    sz_ss, sz_rs, sp_ss, sp_rs, nz_ss, nz_rs, np_ss, np_rs,
):
    me_z = lax.axis_index("pix")
    me_p = lax.axis_index("par")
    core = lax.rem(me_p, 2)
    chip = me_p // 2
    nchip = npar // 2
    partner = me_p + 1 - 2 * core
    size = obs_ref.shape[0] // GROUPS
    groups = range(GROUPS)
    width = green.shape[3]
    rows = nz * SUB * width // GRID
    own_rows = width // GRID
    edge = 2 * GRID
    z_peers = [flipped(me_z, mask, nz) for mask in far_first(nz)]
    z_from = z_peers[::-1]
    p_peers = [
        2 * lax.rem(chip + i, nchip) + c for i in range(1, nchip) for c in range(2)
    ] + [partner]
    order = [(s, c) for s in range(SUB) for c in z_peers] + [(s, me_z) for s in range(SUB)]

    def load(s, c):
        first = pl.multiple_of((c * SUB + s) * width, width)
        return pltpu.make_async_copy(
            green_hbm.at[:, pl.ds(first, width)], green.at[c, s], load_sem.at[c, s]
        )

    for s, c in order:
        load(s, c).start()

    barrier = pltpu.get_barrier_semaphore()
    for j in range(1, nz):
        pl.semaphore_signal(barrier, inc=1, device_id={"pix": lax.rem(me_z + j, nz)}, device_id_type=MESH)
    for j in range(1, npar):
        pl.semaphore_signal(barrier, inc=1, device_id={"par": lax.rem(me_p + j, npar)}, device_id_type=MESH)

    for g in groups:
        mine = slice(g * size, (g + 1) * size)
        imb[g] = obs_ref[mine]
        r_ref[mine] = obs_ref[mine].astype(jnp.float32)
    im[...] = jnp.zeros_like(im)
    p_ext[...] = jnp.zeros_like(p_ext)
    sp[...] = jnp.zeros_like(sp)
    sz[0] = jnp.zeros_like(sz[0])
    sp_scalar[0] = jnp.zeros_like(sp_scalar[0])
    g_own[...] = jnp.zeros_like(g_own)
    gg_ref[...] = jnp.zeros_like(gg_ref)
    x_ref[...] = jnp.zeros_like(x_ref)

    with jax.named_scope("barrier"):
        pl.semaphore_wait(barrier, nz + npar - 2)

    def z_copy(buf, ssem, rsem, k, g, source, target, *s):
        return pltpu.make_async_remote_copy(
            src_ref=buf.at[(k, g, source, *s)], dst_ref=buf.at[(k, g, source, *s)],
            send_sem=ssem.at[(k, g, target, *s)], recv_sem=rsem.at[(k, g, source, *s)],
            device_id={"pix": target}, device_id_type=MESH,
        )

    def to_z(buf, ssem, rsem, k, g, peer, *s):
        return z_copy(buf, ssem, rsem, k, g, me_z, peer, *s)

    def from_z(buf, ssem, rsem, k, g, peer, *s):
        return z_copy(buf, ssem, rsem, k, g, peer, peer, *s)

    def par_copy(buf, ssem, rsem, k, g, source, target):
        return pltpu.make_async_remote_copy(
            src_ref=buf.at[k, g, source], dst_ref=buf.at[k, g, source],
            send_sem=ssem.at[k, g, target], recv_sem=rsem.at[k, g, source],
            device_id={"par": target}, device_id_type=MESH,
        )

    def to_par(buf, ssem, rsem, k, g, peer):
        return par_copy(buf, ssem, rsem, k, g, me_p, peer)

    def from_par(buf, ssem, rsem, k, g, peer):
        return par_copy(buf, ssem, rsem, k, g, peer, peer)

    image_sq = (sz, sz_ss, sz_rs)
    smooth_sq = (sp_scalar, sp_ss, sp_rs)
    pix_sq = (nz_scalar, nz_ss, nz_rs)
    par_sq = (npar_scalar, np_ss, np_rs)
    gathered = (ag, ag_ss, ag_rs)
    images = (h_recv, h_ss, h_rs)

    def total_row(parts):
        value = parts[0]
        for part in parts[1:]:
            value = value + part
        return value

    def z_row(buf, k, g):
        return total_row([buf[k, g, i, 0:1] for i in range(nz)])

    def par_row(buf, k, g):
        return total_row([buf[k, g, i, 0:1] for i in range(npar)])

    def send_image_sq(k, g):
        image = im[g]
        row = to_row(jnp.sum(image * image, axis=1, keepdims=True))
        sz[k, g, me_z] = jnp.broadcast_to(row, (8, LANES))
        for peer in z_peers:
            to_z(*image_sq, k, g, peer).start()

    def send_smooth_sq(k, g):
        square = jnp.zeros((size, GRID), jnp.float32)
        for i in range(rows + 2):
            line = stencil(
                p_ext[g, :, i * GRID:(i + 1) * GRID],
                p_ext[g, :, (i + 1) * GRID:(i + 2) * GRID],
                p_ext[g, :, (i + 2) * GRID:(i + 3) * GRID],
            )
            if i == 0:
                line = jnp.where(me_p == 0, 0.0, line)
            elif i == rows + 1:
                line = jnp.where(me_p == npar - 1, 0.0, line)
            else:
                square = square + line * line
            sp[g, :, i * GRID:(i + 1) * GRID] = line
        row = to_row(jnp.sum(square, axis=1, keepdims=True))
        sp_scalar[k, g, me_p] = jnp.broadcast_to(row, (8, LANES))
        for peer in p_peers:
            to_par(*smooth_sq, k, g, peer).start()

    def wait_curvature(k, g):
        for peer in p_peers:
            from_par(*smooth_sq, k, g, peer).wait_recv()
        for peer in z_from:
            from_z(*image_sq, k, g, peer).wait_recv()

    def step_row(k, g):
        return gg_ref[g, 0:1] / (z_row(sz, k, g) + par_row(sp_scalar, k, g))

    def apply_step(step, g):
        mine = slice(g * size, (g + 1) * size)
        x_ref[mine] += step * p_ext[g, :, edge:edge + rows * GRID]
        r_ref[mine] -= step * im[g]

    def finish_curvature(k, g):
        for peer in z_peers:
            to_z(*image_sq, k, g, peer).wait_send()
        for peer in p_peers:
            to_par(*smooth_sq, k, g, peer).wait_send()

    def rs_copy(k, g, target, s):
        return pltpu.make_async_remote_copy(
            src_ref=rs_send.at[k, g, target, s], dst_ref=rs_recv.at[k, g, me_z, s],
            send_sem=rs_ss.at[k, g, target, s], recv_sem=rs_rs.at[k, g, me_z, s],
            device_id={"pix": target}, device_id_type=MESH,
        )

    def rs_from(k, g, source, s):
        return pltpu.make_async_remote_copy(
            src_ref=rs_send.at[k, g, source, s], dst_ref=rs_recv.at[k, g, source, s],
            send_sem=rs_ss.at[k, g, source, s], recv_sem=rs_rs.at[k, g, source, s],
            device_id={"pix": source}, device_id_type=MESH,
        )

    up = lax.rem(me_p + 1, npar)
    down = lax.rem(me_p + npar - 1, npar)

    def halo_copies(k, g):
        return (
            pltpu.make_async_remote_copy(
                src_ref=ag.at[k, g, nz - 1, SUB - 1, :, pl.ds(width - edge, edge)],
                dst_ref=halo.at[k, g, 0],
                send_sem=halo_ss.at[k, g, 0], recv_sem=halo_rs.at[k, g, 0],
                device_id={"par": up}, device_id_type=MESH,
            ),
            pltpu.make_async_remote_copy(
                src_ref=ag.at[k, g, 0, 0, :, pl.ds(0, edge)],
                dst_ref=halo.at[k, g, 1],
                send_sem=halo_ss.at[k, g, 1], recv_sem=halo_rs.at[k, g, 1],
                device_id={"par": down}, device_id_type=MESH,
            ),
        )

    def scatter(k, g, loading=False):
        vector = imb[g]

        def backward(s, c):
            if loading:
                load(s, c).wait()
            return jnp.dot(vector, green[c, s], preferred_element_type=jnp.float32)

        with jax.named_scope("bwd%d" % g):
            for s in range(SUB):
                for peer in z_peers:
                    rs_send[k, g, peer, s] = backward(s, peer).astype(jnp.bfloat16)
                    rs_copy(k, g, peer, s).start()
        with jax.named_scope("own%d" % g):
            for s in range(SUB):
                base = (me_z * SUB + s) * own_rows
                lines = []
                for i in range(own_rows):
                    lines.append(stencil(*[
                        sp[g, :, pl.ds(pl.multiple_of((base + i + d) * GRID, GRID), GRID)]
                        for d in range(3)
                    ]))
                own_part[g, s] = backward(s, me_z) + jnp.concatenate(lines, axis=1)

    def forward(k, g, s, c):
        return jnp.dot(ag[k, g, c, s], green_t[c, s], preferred_element_type=jnp.float32)

    def gather(k, g):
        with jax.named_scope("curv%d" % g):
            @pl.when(k > 0)
            def _():
                wait_curvature(k, g)

            step = to_column(jnp.where(k == 0, -1.0, step_row(k, g)), size)
        square = jnp.zeros((size, 1), jnp.float32)
        for s in range(SUB):
            with jax.named_scope("rs%d" % g):
                for source in z_from:
                    rs_from(k, g, source, s).wait_recv()
            with jax.named_scope("upd%d" % g):
                fresh = own_part[g, s]
                for source in z_from:
                    fresh = fresh + rs_recv[k, g, source, s].astype(jnp.float32)
                gradient = g_own[g, s] - step * fresh
                g_own[g, s] = gradient
                ag[k, g, me_z, s] = gradient.astype(jnp.bfloat16)
                for peer in z_peers:
                    to_z(*gathered, k, g, peer, s).start()
                square = square + jnp.sum(gradient * gradient, axis=1, keepdims=True)
            with jax.named_scope("fown%d" % g):
                image = forward(k, g, s, me_z)
                own_image[g] = image if s == 0 else own_image[g] + image
        with jax.named_scope("app%d" % g):
            nz_scalar[k, g, me_z] = jnp.broadcast_to(to_row(square), (8, LANES))
            for peer in z_peers:
                to_z(*pix_sq, k, g, peer).start()
            apply_step(step, g)

    def forward_rest(k, g):
        image = own_image[g]
        with jax.named_scope("frest%d" % g):
            turns = [(s, source) for s in range(SUB) for source in z_from]
            for i, (s, source) in enumerate(turns):
                from_z(*gathered, k, g, source, s).wait_recv()
                if i + 1 == len(turns):
                    for copy in halo_copies(k, g):
                        copy.start()
                image = image + forward(k, g, s, source)
                if i + 1 == len(z_from):
                    for source in z_from:
                        from_z(*pix_sq, k, g, source).wait_recv()
                    npar_scalar[k, g, me_p] = jnp.broadcast_to(z_row(nz_scalar, k, g), (8, LANES))
                    for peer in p_peers:
                        to_par(*par_sq, k, g, peer).start()
        with jax.named_scope("hsend%d" % g):
            h_recv[k, g, me_p] = image.astype(jnp.bfloat16)
            for peer in p_peers:
                to_par(*images, k, g, peer).start()

    def advance(k, g):
        with jax.named_scope("npw%d" % g):
            for peer in p_peers:
                from_par(*par_sq, k, g, peer).wait_recv()
            for copy in halo_copies(k, g):
                copy.wait_recv()
        with jax.named_scope("pupd%d" % g):
            fresh_sq = par_row(npar_scalar, k, g)
            ratio = to_column(jnp.where(k == 0, 0.0, fresh_sq / gg_ref[g, 0:1]), size)
            gg_ref[g] = jnp.broadcast_to(fresh_sq, (8, LANES))
            for c in range(nz):
                for s in range(SUB):
                    first = edge + (c * SUB + s) * width
                    where = slice(first, first + width)
                    p_ext[g, :, where] = (
                        ag[k, g, c, s].astype(jnp.float32) + ratio * p_ext[g, :, where]
                    )
            first = jnp.where(me_p == 0, 0.0, halo[k, g, 0].astype(jnp.float32))
            p_ext[g, :, :edge] = first + ratio * p_ext[g, :, :edge]
            last = jnp.where(me_p == npar - 1, 0.0, halo[k, g, 1].astype(jnp.float32))
            p_ext[g, :, edge + rows * GRID:] = last + ratio * p_ext[g, :, edge + rows * GRID:]
            send_smooth_sq(k + 1, g)
        with jax.named_scope("hw%d" % g):
            for peer in p_peers:
                from_par(*images, k, g, peer).wait_recv()
        with jax.named_scope("im%d" % g):
            part = h_recv[k, g, 0].astype(jnp.float32)
            for i in range(1, npar):
                part = part + h_recv[k, g, i].astype(jnp.float32)
            image = part + ratio * im[g]
            im[g] = image
            imb[g] = image.astype(jnp.bfloat16)
            send_image_sq(k + 1, g)

    def finish_sends(k, g):
        for peer in z_peers:
            for s in range(SUB):
                rs_copy(k, g, peer, s).wait_send()
            to_z(*pix_sq, k, g, peer).wait_send()
        for s in range(SUB):
            for peer in z_peers:
                to_z(*gathered, k, g, peer, s).wait_send()
        for copy in halo_copies(k, g):
            copy.wait_send()
        for peer in p_peers:
            to_par(*par_sq, k, g, peer).wait_send()
            to_par(*images, k, g, peer).wait_send()
        finish_curvature(k + 1, g)

    scatter(0, 0, loading=True)
    with jax.named_scope("transp"):
        for s, c in order:
            green_t[c, s] = green[c, s].T

    @pl.loop(0, ITERS)
    def _(k):
        gather(k, 0)

        @pl.when(k > 0)
        def _():
            advance(k - 1, 1)

        scatter(k, 1)

        @pl.when(k > 0)
        def _():
            finish_sends(k - 1, 1)

        forward_rest(k, 0)
        gather(k, 1)
        advance(k, 0)

        @pl.when(k + 1 < ITERS)
        def _():
            scatter(k + 1, 0)

        forward_rest(k, 1)
        finish_sends(k, 0)

    with jax.named_scope("final"):
        wait_curvature(ITERS, 0)
        apply_step(to_column(step_row(ITERS, 0), size), 0)
    advance(ITERS - 1, 1)
    with jax.named_scope("final2"):
        finish_sends(ITERS - 1, 1)
        wait_curvature(ITERS, 1)
        apply_step(to_column(step_row(ITERS, 1), size), 1)


def finish_kernel(x_ref, r_ref, x_out, r_out, x_sem, r_sem):
    copies = (
        pltpu.make_async_copy(x_ref, x_out, x_sem),
        pltpu.make_async_copy(r_ref, r_out, r_sem),
    )
    for copy in copies:
        copy.start()
    for copy in copies:
        copy.wait()


def finish(x, r):
    vmem = pl.BlockSpec(memory_space=pltpu.VMEM)
    space = pl.BlockSpec(memory_space=pl.ANY)
    return pl.pallas_call(
        finish_kernel,
        out_shape=(jax.ShapeDtypeStruct(x.shape, x.dtype), jax.ShapeDtypeStruct(r.shape, r.dtype)),
        in_specs=[vmem, vmem],
        out_specs=(space, space),
        scratch_shapes=[pltpu.SemaphoreType.DMA, pltpu.SemaphoreType.DMA],
    )(x, r)


def on_device_kernel(nz, npar, green_matrix, observed):
    sets, pixels = observed.shape
    cells = green_matrix.shape[1]
    width = cells // (nz * SUB)
    size = sets // GROUPS
    bf16, f32 = jnp.bfloat16, jnp.float32
    dma = pltpu.SemaphoreType.DMA
    n = ITERS
    vmem = pl.BlockSpec(memory_space=pltpu.VMEM)
    return pl.pallas_call(
        functools.partial(cgls_kernel, nz, npar),
        out_shape=(
            jax.ShapeDtypeStruct((sets, cells), f32),
            jax.ShapeDtypeStruct((sets, pixels), f32),
        ),
        in_specs=[pl.BlockSpec(memory_space=pl.ANY), vmem],
        out_specs=(vmem, vmem),
        scratch_shapes=[
            pltpu.VMEM((nz, SUB, pixels, width), bf16),
            pltpu.VMEM((nz, SUB, width, pixels), bf16),
            pltpu.VMEM((GROUPS, size, pixels), bf16),
            pltpu.VMEM((GROUPS, size, pixels), f32),
            pltpu.VMEM((GROUPS, size, pixels), f32),
            pltpu.VMEM((GROUPS, size, cells + 4 * GRID), f32),
            pltpu.VMEM((GROUPS, size, cells + 2 * GRID), f32),
            pltpu.VMEM((GROUPS, SUB, size, width), f32),
            pltpu.VMEM((GROUPS, SUB, size, width), f32),
            pltpu.VMEM((GROUPS, 8, LANES), f32),
            pltpu.VMEM((n, GROUPS, nz, SUB, size, width), bf16),
            pltpu.VMEM((n, GROUPS, nz, SUB, size, width), bf16),
            pltpu.VMEM((n, GROUPS, nz, SUB, size, width), bf16),
            pltpu.VMEM((n, GROUPS, npar, size, pixels), bf16),
            pltpu.VMEM((n, GROUPS, 2, size, 2 * GRID), bf16),
            pltpu.VMEM((n + 1, GROUPS, nz, 8, LANES), f32),
            pltpu.VMEM((n + 1, GROUPS, npar, 8, LANES), f32),
            pltpu.VMEM((n, GROUPS, nz, 8, LANES), f32),
            pltpu.VMEM((n, GROUPS, npar, 8, LANES), f32),
            dma((nz, SUB)),
            dma((n, GROUPS, nz, SUB)), dma((n, GROUPS, nz, SUB)),
            dma((n, GROUPS, nz, SUB)), dma((n, GROUPS, nz, SUB)),
            dma((n, GROUPS, npar)), dma((n, GROUPS, npar)),
            dma((n, GROUPS, 2)), dma((n, GROUPS, 2)),
            dma((n + 1, GROUPS, nz)), dma((n + 1, GROUPS, nz)),
            dma((n + 1, GROUPS, npar)), dma((n + 1, GROUPS, npar)),
            dma((n, GROUPS, nz)), dma((n, GROUPS, nz)),
            dma((n, GROUPS, npar)), dma((n, GROUPS, npar)),
        ],
        compiler_params=pltpu.CompilerParams(
            collective_id=0, has_side_effects=True, vmem_limit_bytes=60 * 1024 * 1024
        ),
    )(green_matrix, observed)


def solution(mesh):
    nz, npar = mesh.shape["pix"], mesh.shape["par"]

    def step(green_matrix, observed):
        sets, cells = observed.shape[0], green_matrix.shape[1]
        width = cells // (nz * SUB)
        fits = cells % (nz * SUB * GRID) == 0 and width >= 2 * GRID and nz & (nz - 1) == 0
        if fits and nz > 1 and npar % 2 == 0 and sets % 32 == 0 and sets <= LANES:
            return finish(*on_device_kernel(nz, npar, green_matrix, observed))
        return on_device(green_matrix, observed)

    return jax.shard_map(
        step,
        mesh=mesh,
        in_specs=(P("pix", "par"), P("parts", "pix")),
        out_specs=(P("parts", "par"), P("parts", "pix")),
        check_vma=False,
    )
```

```python
import functools

import jax
import jax.numpy as jnp
from jax import lax
from jax.experimental import pallas as pl
from jax.experimental.pallas import tpu as pltpu
from jax.sharding import PartitionSpec as P

GRID = 128
ITERS = 5
LANES = 128
SUB = 2
GROUPS = 2
STOPS = (3, 6)


def padded_2(block, sides, width):
    for axis, dim in sides:
        count = lax.axis_size(axis)
        forward = [(i, i + 1) for i in range(count - 1)]
        backward = [(target, source) for source, target in forward]
        low = lax.ppermute(
            lax.slice_in_dim(block, block.shape[dim] - width, None, axis=dim), axis, forward
        )
        high = lax.ppermute(lax.slice_in_dim(block, 0, width, axis=dim), axis, backward)
        block = jnp.concatenate([low, block, high], axis=dim)
    return block


def smooth(values):
    set_count = values.shape[0]
    grid_rows = values.shape[1] // GRID
    tiles = values.reshape(set_count, grid_rows, GRID)
    padded = padded_2(tiles, (("par", 1),), 1)
    padded = jnp.pad(padded, ((0, 0), (0, 0), (1, 1)))
    beside_all = (
        padded[:, 2:, 1:-1] + padded[:, :-2, 1:-1] + padded[:, 1:-1, 2:] + padded[:, 1:-1, :-2]
    )
    return (0.25 * (4.0 * tiles - beside_all)).reshape(set_count, grid_rows * GRID)


def forward(rounded, green_matrix):
    partial_value = lax.dot_general(
        rounded, green_matrix, (((1,), (1,)), ((), ())), preferred_element_type=jnp.float32
    )
    return lax.psum(partial_value, "par")


def curvatures(image, smoothed):
    local_image = jnp.sum(image * image, axis=1)
    local_smooth = jnp.sum(smoothed * smoothed, axis=1)
    image_sq = lax.psum(local_image, "pix")
    smooth_sq = lax.psum(local_smooth, "par")
    return image_sq + smooth_sq


def backward_sum(rounded, green_matrix):
    return lax.psum(jnp.dot(rounded, green_matrix, preferred_element_type=jnp.float32), "pix")


def column_squares(gradient):
    return lax.psum(jnp.sum(gradient * gradient, axis=1), "par")


def on_device(green_matrix, observed):
    set_count = observed.shape[0]
    tile_cells = green_matrix.shape[1]
    residual = observed.astype(jnp.float32)
    gradient = backward_sum(observed, green_matrix)
    grad_sq = column_squares(gradient)
    direction = gradient
    solution = jnp.zeros((set_count, tile_cells), jnp.float32)
    smooth_res = jnp.zeros((set_count, tile_cells), jnp.float32)
    for sweep in range(ITERS):
        rounded = direction.astype(jnp.bfloat16)
        image = forward(rounded, green_matrix)
        smoothed = smooth(lax.optimization_barrier(rounded).astype(jnp.float32))
        step_len = (grad_sq / curvatures(image, smoothed))[:, None]
        solution = solution + step_len * direction
        residual = residual - step_len * image
        smooth_res = smooth_res - step_len * smoothed
        if sweep + 1 < ITERS:
            gradient = backward_sum(residual.astype(jnp.bfloat16), green_matrix) + smooth(
                smooth_res
            )
            fresh_sq = column_squares(gradient)
            direction = gradient + (fresh_sq / grad_sq)[:, None] * direction
            grad_sq = fresh_sq
    return (solution, residual)


MESH = pl.DeviceIdType.MESH


def to_row(column):
    count = column.shape[0]
    eye = lax.broadcasted_iota(jnp.int32, (count, LANES), 0) == lax.broadcasted_iota(
        jnp.int32, (count, LANES), 1
    )
    return jnp.sum(jnp.where(eye, jnp.broadcast_to(column, (count, LANES)), 0.0), axis=0, keepdims=True)


def to_column(row, count):
    eye = lax.broadcasted_iota(jnp.int32, (count, LANES), 0) == lax.broadcasted_iota(
        jnp.int32, (count, LANES), 1
    )
    return jnp.sum(jnp.where(eye, jnp.broadcast_to(row, (count, LANES)), 0.0), axis=1, keepdims=True)


def flipped(index, mask, count):
    value, bit = 0, 1
    while bit < count:
        digit = lax.rem(index // bit, 2)
        value = value + bit * (1 - digit if mask & bit else digit)
        bit *= 2
    return value


def far_first(count):
    masks = []
    bit = count // 2
    while bit:
        masks += range(2 * bit - 1, bit - 1, -1)
        bit //= 2
    return masks


def stencil(above, here, below):
    lane = lax.broadcasted_iota(jnp.int32, here.shape, 1)
    left = jnp.where(lane == 0, 0.0, pltpu.roll(here, 1, 1))
    right = jnp.where(lane == GRID - 1, 0.0, pltpu.roll(here, GRID - 1, 1))
    return here - 0.25 * (above + below + left + right)


def cgls_kernel(
    nz, npar,
    green_hbm, obs_hbm, x_ref, r_ref,
    obs_ref, green, green_t, imb, im, own_image, p_ext, sp, g_own, own_part, gg_ref,
    rs_send, rs_recv, ag, h_recv, halo,
    sz, sp_scalar, nz_scalar, npar_scalar,
    obs_sem, load_sem, rs_ss, rs_rs, ag_ss, ag_rs, h_ss, h_rs, halo_ss, halo_rs,
    sz_ss, sz_rs, sp_ss, sp_rs, nz_ss, nz_rs, np_ss, np_rs,
):
    me_z = lax.axis_index("pix")
    me_p = lax.axis_index("par")
    core = lax.rem(me_p, 2)
    chip = me_p // 2
    nchip = npar // 2
    partner = me_p + 1 - 2 * core
    size = obs_ref.shape[0] // GROUPS
    groups = range(GROUPS)
    width = green.shape[3]
    rows = nz * SUB * width // GRID
    own_rows = width // GRID
    edge = 2 * GRID
    z_peers = [flipped(me_z, mask, nz) for mask in far_first(nz)]
    z_from = z_peers[::-1]
    p_peers = [
        2 * lax.rem(chip + i, nchip) + c for i in range(1, nchip) for c in range(2)
    ] + [partner]
    order = [(s, c) for s in range(SUB) for c in z_peers] + [(s, me_z) for s in range(SUB)]

    def load(s, c):
        first = pl.multiple_of((c * SUB + s) * width, width)
        return pltpu.make_async_copy(
            green_hbm.at[:, pl.ds(first, width)], green.at[c, s], load_sem.at[c, s]
        )

    obs_copy = pltpu.make_async_copy(obs_hbm, obs_ref, obs_sem)
    obs_copy.start()
    for s, c in order:
        load(s, c).start()

    barrier = pltpu.get_barrier_semaphore()
    for j in range(1, nz):
        pl.semaphore_signal(barrier, inc=1, device_id={"pix": lax.rem(me_z + j, nz)}, device_id_type=MESH)
    for j in range(1, npar):
        pl.semaphore_signal(barrier, inc=1, device_id={"par": lax.rem(me_p + j, npar)}, device_id_type=MESH)

    im[...] = jnp.zeros_like(im)
    p_ext[...] = jnp.zeros_like(p_ext)
    sp[...] = jnp.zeros_like(sp)
    sz[0] = jnp.zeros_like(sz[0])
    sp_scalar[0] = jnp.zeros_like(sp_scalar[0])
    g_own[...] = jnp.zeros_like(g_own)
    gg_ref[...] = jnp.zeros_like(gg_ref)
    x_ref[...] = jnp.zeros_like(x_ref)
    obs_copy.wait()
    for g in groups:
        mine = slice(g * size, (g + 1) * size)
        imb[g] = obs_ref[mine]
        r_ref[mine] = obs_ref[mine].astype(jnp.float32)

    with jax.named_scope("barrier"):
        pl.semaphore_wait(barrier, nz + npar - 2)

    def z_copy(buf, ssem, rsem, k, g, source, target, *s):
        return pltpu.make_async_remote_copy(
            src_ref=buf.at[(k, g, source, *s)], dst_ref=buf.at[(k, g, source, *s)],
            send_sem=ssem.at[(k, g, target, *s)], recv_sem=rsem.at[(k, g, source, *s)],
            device_id={"pix": target}, device_id_type=MESH,
        )

    def to_z(buf, ssem, rsem, k, g, peer, *s):
        return z_copy(buf, ssem, rsem, k, g, me_z, peer, *s)

    def from_z(buf, ssem, rsem, k, g, peer, *s):
        return z_copy(buf, ssem, rsem, k, g, peer, peer, *s)

    def par_copy(buf, ssem, rsem, k, g, source, target):
        return pltpu.make_async_remote_copy(
            src_ref=buf.at[k, g, source], dst_ref=buf.at[k, g, source],
            send_sem=ssem.at[k, g, target], recv_sem=rsem.at[k, g, source],
            device_id={"par": target}, device_id_type=MESH,
        )

    def to_par(buf, ssem, rsem, k, g, peer):
        return par_copy(buf, ssem, rsem, k, g, me_p, peer)

    def from_par(buf, ssem, rsem, k, g, peer):
        return par_copy(buf, ssem, rsem, k, g, peer, peer)

    image_sq = (sz, sz_ss, sz_rs)
    smooth_sq = (sp_scalar, sp_ss, sp_rs)
    pix_sq = (nz_scalar, nz_ss, nz_rs)
    par_sq = (npar_scalar, np_ss, np_rs)
    gathered = (ag, ag_ss, ag_rs)
    images = (h_recv, h_ss, h_rs)

    def total_row(parts):
        value = parts[0]
        for part in parts[1:]:
            value = value + part
        return value

    def z_row(buf, k, g):
        return total_row([buf[k, g, i] for i in range(nz)])

    def par_row(buf, k, g):
        return total_row([buf[k, g, i] for i in range(npar)])

    def send_image_sq(k, g):
        image = im[g]
        row = to_row(jnp.sum(image * image, axis=1, keepdims=True))
        sz[k, g, me_z] = row
        for peer in z_peers:
            to_z(*image_sq, k, g, peer).start()

    def send_smooth_sq(k, g):
        square = jnp.zeros((size, GRID), jnp.float32)
        for i in range(rows + 2):
            line = stencil(
                p_ext[g, :, i * GRID:(i + 1) * GRID],
                p_ext[g, :, (i + 1) * GRID:(i + 2) * GRID],
                p_ext[g, :, (i + 2) * GRID:(i + 3) * GRID],
            )
            if i == 0:
                line = jnp.where(me_p == 0, 0.0, line)
            elif i == rows + 1:
                line = jnp.where(me_p == npar - 1, 0.0, line)
            else:
                square = square + line * line
            sp[g, :, i * GRID:(i + 1) * GRID] = line
        row = to_row(jnp.sum(square, axis=1, keepdims=True))
        sp_scalar[k, g, me_p] = row
        for peer in p_peers:
            to_par(*smooth_sq, k, g, peer).start()

    def wait_curvature(k, g):
        for peer in p_peers:
            from_par(*smooth_sq, k, g, peer).wait_recv()
        for peer in z_from:
            from_z(*image_sq, k, g, peer).wait_recv()

    def step_row(k, g):
        return gg_ref[g] / (z_row(sz, k, g) + par_row(sp_scalar, k, g))

    def apply_step(step, g):
        mine = slice(g * size, (g + 1) * size)
        x_ref[mine] += step * p_ext[g, :, edge:edge + rows * GRID]
        r_ref[mine] -= step * im[g]

    def finish_curvature(k, g):
        for peer in z_peers:
            to_z(*image_sq, k, g, peer).wait_send()
        for peer in p_peers:
            to_par(*smooth_sq, k, g, peer).wait_send()

    def rs_copy(k, g, target, s):
        return pltpu.make_async_remote_copy(
            src_ref=rs_send.at[k, g, target, s], dst_ref=rs_recv.at[k, g, me_z, s],
            send_sem=rs_ss.at[k, g, target, s], recv_sem=rs_rs.at[k, g, me_z, s],
            device_id={"pix": target}, device_id_type=MESH,
        )

    def rs_from(k, g, source, s):
        return pltpu.make_async_remote_copy(
            src_ref=rs_send.at[k, g, source, s], dst_ref=rs_recv.at[k, g, source, s],
            send_sem=rs_ss.at[k, g, source, s], recv_sem=rs_rs.at[k, g, source, s],
            device_id={"pix": source}, device_id_type=MESH,
        )

    up = lax.rem(me_p + 1, npar)
    down = lax.rem(me_p + npar - 1, npar)

    def halo_copies(k, g):
        return (
            pltpu.make_async_remote_copy(
                src_ref=ag.at[k, g, nz - 1, SUB - 1, :, pl.ds(width - edge, edge)],
                dst_ref=halo.at[k, g, 0],
                send_sem=halo_ss.at[k, g, 0], recv_sem=halo_rs.at[k, g, 0],
                device_id={"par": up}, device_id_type=MESH,
            ),
            pltpu.make_async_remote_copy(
                src_ref=ag.at[k, g, 0, 0, :, pl.ds(0, edge)],
                dst_ref=halo.at[k, g, 1],
                send_sem=halo_ss.at[k, g, 1], recv_sem=halo_rs.at[k, g, 1],
                device_id={"par": down}, device_id_type=MESH,
            ),
        )

    def scatter(k, g, loading=False):
        vector = imb[g]

        def backward(s, c):
            if loading:
                load(s, c).wait()
            return jnp.dot(vector, green[c, s], preferred_element_type=jnp.float32)

        with jax.named_scope("bwd%d" % g):
            turns = [(s, peer) for s in range(SUB) for peer in z_peers]
            ready = backward(*turns[0])
            for i, (s, peer) in enumerate(turns):
                value = ready
                if i + 1 < len(turns):
                    ready = backward(*turns[i + 1])
                rs_send[k, g, peer, s] = value.astype(jnp.bfloat16)
                rs_copy(k, g, peer, s).start()
        with jax.named_scope("own%d" % g):
            for s in range(SUB):
                base = (me_z * SUB + s) * own_rows
                lines = []
                for i in range(own_rows):
                    lines.append(stencil(*[
                        sp[g, :, pl.ds(pl.multiple_of((base + i + d) * GRID, GRID), GRID)]
                        for d in range(3)
                    ]))
                own_part[g, s] = backward(s, me_z) + jnp.concatenate(lines, axis=1)

    def forward(k, g, s, c):
        return jnp.dot(ag[k, g, c, s], green_t[c, s], preferred_element_type=jnp.float32)

    def gather(k, g):
        with jax.named_scope("curv%d" % g):
            @pl.when(k > 0)
            def _():
                wait_curvature(k, g)

            step = to_column(jnp.where(k == 0, -1.0, step_row(k, g)), size)
        square = jnp.zeros((size, 1), jnp.float32)
        for s in range(SUB):
            with jax.named_scope("rs%d" % g):
                for source in z_from:
                    rs_from(k, g, source, s).wait_recv()
            with jax.named_scope("upd%d" % g):
                fresh = own_part[g, s]
                for source in z_from:
                    fresh = fresh + rs_recv[k, g, source, s].astype(jnp.float32)
                gradient = g_own[g, s] - step * fresh
                g_own[g, s] = gradient
                ag[k, g, me_z, s] = gradient.astype(jnp.bfloat16)
                for peer in z_peers:
                    to_z(*gathered, k, g, peer, s).start()
                square = square + jnp.sum(gradient * gradient, axis=1, keepdims=True)
            with jax.named_scope("fown%d" % g):
                image = forward(k, g, s, me_z)
                own_image[g] = image if s == 0 else own_image[g] + image
        with jax.named_scope("app%d" % g):
            nz_scalar[k, g, me_z] = to_row(square)
            for peer in z_peers:
                to_z(*pix_sq, k, g, peer).start()
            apply_step(step, g)

    def forward_rest(k, g):
        image = own_image[g]
        with jax.named_scope("frest%d" % g):
            turns = [(s, source) for s in range(SUB) for source in z_from]
            for i, stop in enumerate(STOPS):
                batch = turns[STOPS[i - 1] if i else 0:stop]
                for s, source in batch:
                    from_z(*gathered, k, g, source, s).wait_recv()
                if i + 1 == len(STOPS):
                    for copy in halo_copies(k, g):
                        copy.start()
                for s, source in batch:
                    image = image + forward(k, g, s, source)
                if i == 0:
                    for source in z_from:
                        from_z(*pix_sq, k, g, source).wait_recv()
                    npar_scalar[k, g, me_p] = z_row(nz_scalar, k, g)
                    for peer in p_peers:
                        to_par(*par_sq, k, g, peer).start()
        with jax.named_scope("hsend%d" % g):
            h_recv[k, g, me_p] = image.astype(jnp.bfloat16)
            for peer in p_peers:
                to_par(*images, k, g, peer).start()

    def advance(k, g):
        with jax.named_scope("npw%d" % g):
            for peer in p_peers:
                from_par(*par_sq, k, g, peer).wait_recv()
            for copy in halo_copies(k, g):
                copy.wait_recv()
        with jax.named_scope("pupd%d" % g):
            fresh_sq = par_row(npar_scalar, k, g)
            ratio = to_column(jnp.where(k == 0, 0.0, fresh_sq / gg_ref[g]), size)
            gg_ref[g] = fresh_sq
            for c in range(nz):
                for s in range(SUB):
                    first = edge + (c * SUB + s) * width
                    where = slice(first, first + width)
                    p_ext[g, :, where] = (
                        ag[k, g, c, s].astype(jnp.float32) + ratio * p_ext[g, :, where]
                    )
            first = jnp.where(me_p == 0, 0.0, halo[k, g, 0].astype(jnp.float32))
            p_ext[g, :, :edge] = first + ratio * p_ext[g, :, :edge]
            last = jnp.where(me_p == npar - 1, 0.0, halo[k, g, 1].astype(jnp.float32))
            p_ext[g, :, edge + rows * GRID:] = last + ratio * p_ext[g, :, edge + rows * GRID:]
            send_smooth_sq(k + 1, g)
        with jax.named_scope("hw%d" % g):
            for peer in p_peers:
                from_par(*images, k, g, peer).wait_recv()
        with jax.named_scope("im%d" % g):
            part = h_recv[k, g, 0].astype(jnp.float32)
            for i in range(1, npar):
                part = part + h_recv[k, g, i].astype(jnp.float32)
            image = part + ratio * im[g]
            im[g] = image
            imb[g] = image.astype(jnp.bfloat16)
            send_image_sq(k + 1, g)

    def finish_sends(k, g):
        for peer in z_peers:
            for s in range(SUB):
                rs_copy(k, g, peer, s).wait_send()
            to_z(*pix_sq, k, g, peer).wait_send()
        for s in range(SUB):
            for peer in z_peers:
                to_z(*gathered, k, g, peer, s).wait_send()
        for copy in halo_copies(k, g):
            copy.wait_send()
        for peer in p_peers:
            to_par(*par_sq, k, g, peer).wait_send()
            to_par(*images, k, g, peer).wait_send()
        finish_curvature(k + 1, g)

    scatter(0, 0, loading=True)
    with jax.named_scope("transp"):
        for s, c in order:
            green_t[c, s] = green[c, s].T

    @pl.loop(0, ITERS)
    def _(k):
        gather(k, 0)

        @pl.when(k > 0)
        def _():
            advance(k - 1, 1)

        scatter(k, 1)

        @pl.when(k > 0)
        def _():
            finish_sends(k - 1, 1)

        forward_rest(k, 0)
        gather(k, 1)
        advance(k, 0)

        @pl.when(k + 1 < ITERS)
        def _():
            scatter(k + 1, 0)

        forward_rest(k, 1)
        finish_sends(k, 0)

    with jax.named_scope("final"):
        wait_curvature(ITERS, 0)
        apply_step(to_column(step_row(ITERS, 0), size), 0)
    advance(ITERS - 1, 1)
    with jax.named_scope("final2"):
        finish_sends(ITERS - 1, 1)
        wait_curvature(ITERS, 1)
        apply_step(to_column(step_row(ITERS, 1), size), 1)


def finish_kernel(x_ref, r_ref, x_out, r_out, x_sem, r_sem):
    copies = (
        pltpu.make_async_copy(x_ref, x_out, x_sem),
        pltpu.make_async_copy(r_ref, r_out, r_sem),
    )
    for copy in copies:
        copy.start()
    for copy in copies:
        copy.wait()


def finish(x, r):
    vmem = pl.BlockSpec(memory_space=pltpu.VMEM)
    space = pl.BlockSpec(memory_space=pl.ANY)
    return pl.pallas_call(
        finish_kernel,
        out_shape=(jax.ShapeDtypeStruct(x.shape, x.dtype), jax.ShapeDtypeStruct(r.shape, r.dtype)),
        in_specs=[vmem, vmem],
        out_specs=(space, space),
        scratch_shapes=[pltpu.SemaphoreType.DMA, pltpu.SemaphoreType.DMA],
    )(x, r)


def on_device_kernel(nz, npar, green_matrix, observed):
    sets, pixels = observed.shape
    cells = green_matrix.shape[1]
    width = cells // (nz * SUB)
    size = sets // GROUPS
    bf16, f32 = jnp.bfloat16, jnp.float32
    dma = pltpu.SemaphoreType.DMA
    n = ITERS
    vmem = pl.BlockSpec(memory_space=pltpu.VMEM)
    return pl.pallas_call(
        functools.partial(cgls_kernel, nz, npar),
        out_shape=(
            jax.ShapeDtypeStruct((sets, cells), f32),
            jax.ShapeDtypeStruct((sets, pixels), f32),
        ),
        in_specs=[pl.BlockSpec(memory_space=pl.ANY), pl.BlockSpec(memory_space=pl.ANY)],
        out_specs=(vmem, vmem),
        scratch_shapes=[
            pltpu.VMEM((sets, pixels), bf16),
            pltpu.VMEM((nz, SUB, pixels, width), bf16),
            pltpu.VMEM((nz, SUB, width, pixels), bf16),
            pltpu.VMEM((GROUPS, size, pixels), bf16),
            pltpu.VMEM((GROUPS, size, pixels), f32),
            pltpu.VMEM((GROUPS, size, pixels), f32),
            pltpu.VMEM((GROUPS, size, cells + 4 * GRID), f32),
            pltpu.VMEM((GROUPS, size, cells + 2 * GRID), f32),
            pltpu.VMEM((GROUPS, SUB, size, width), f32),
            pltpu.VMEM((GROUPS, SUB, size, width), f32),
            pltpu.VMEM((GROUPS, 1, LANES), f32),
            pltpu.VMEM((n, GROUPS, nz, SUB, size, width), bf16),
            pltpu.VMEM((n, GROUPS, nz, SUB, size, width), bf16),
            pltpu.VMEM((n, GROUPS, nz, SUB, size, width), bf16),
            pltpu.VMEM((n, GROUPS, npar, size, pixels), bf16),
            pltpu.VMEM((n, GROUPS, 2, size, 2 * GRID), bf16),
            pltpu.VMEM((n + 1, GROUPS, nz, 1, LANES), f32),
            pltpu.VMEM((n + 1, GROUPS, npar, 1, LANES), f32),
            pltpu.VMEM((n, GROUPS, nz, 1, LANES), f32),
            pltpu.VMEM((n, GROUPS, npar, 1, LANES), f32),
            dma,
            dma((nz, SUB)),
            dma((n, GROUPS, nz, SUB)), dma((n, GROUPS, nz, SUB)),
            dma((n, GROUPS, nz, SUB)), dma((n, GROUPS, nz, SUB)),
            dma((n, GROUPS, npar)), dma((n, GROUPS, npar)),
            dma((n, GROUPS, 2)), dma((n, GROUPS, 2)),
            dma((n + 1, GROUPS, nz)), dma((n + 1, GROUPS, nz)),
            dma((n + 1, GROUPS, npar)), dma((n + 1, GROUPS, npar)),
            dma((n, GROUPS, nz)), dma((n, GROUPS, nz)),
            dma((n, GROUPS, npar)), dma((n, GROUPS, npar)),
        ],
        compiler_params=pltpu.CompilerParams(
            collective_id=0, has_side_effects=True, vmem_limit_bytes=60 * 1024 * 1024
        ),
    )(green_matrix, observed)


def solution(mesh):
    nz, npar = mesh.shape["pix"], mesh.shape["par"]

    def step(green_matrix, observed):
        sets, cells = observed.shape[0], green_matrix.shape[1]
        width = cells // (nz * SUB)
        fits = cells % (nz * SUB * GRID) == 0 and width >= 2 * GRID and nz & (nz - 1) == 0
        if fits and nz > 1 and npar % 2 == 0 and sets % 32 == 0 and sets <= LANES:
            return finish(*on_device_kernel(nz, npar, green_matrix, observed))
        return on_device(green_matrix, observed)

    return jax.shard_map(
        step,
        mesh=mesh,
        in_specs=(P("pix", "par"), P("parts", "pix")),
        out_specs=(P("parts", "par"), P("parts", "pix")),
        check_vma=False,
    )
```

```python
import functools

import jax
import jax.numpy as jnp
from jax import lax
from jax.experimental import pallas as pl
from jax.experimental.pallas import tpu as pltpu
from jax.sharding import PartitionSpec as P

GRID = 128
ITERS = 5
LANES = 128
SUB = 2
GROUPS = 2
STOPS = (3, 6)


def padded_2(block, sides, width):
    for axis, dim in sides:
        count = lax.axis_size(axis)
        forward = [(i, i + 1) for i in range(count - 1)]
        backward = [(target, source) for source, target in forward]
        low = lax.ppermute(
            lax.slice_in_dim(block, block.shape[dim] - width, None, axis=dim), axis, forward
        )
        high = lax.ppermute(lax.slice_in_dim(block, 0, width, axis=dim), axis, backward)
        block = jnp.concatenate([low, block, high], axis=dim)
    return block


def smooth(values):
    set_count = values.shape[0]
    grid_rows = values.shape[1] // GRID
    tiles = values.reshape(set_count, grid_rows, GRID)
    padded = padded_2(tiles, (("par", 1),), 1)
    padded = jnp.pad(padded, ((0, 0), (0, 0), (1, 1)))
    beside_all = (
        padded[:, 2:, 1:-1] + padded[:, :-2, 1:-1] + padded[:, 1:-1, 2:] + padded[:, 1:-1, :-2]
    )
    return (0.25 * (4.0 * tiles - beside_all)).reshape(set_count, grid_rows * GRID)


def forward(rounded, green_matrix):
    partial_value = lax.dot_general(
        rounded, green_matrix, (((1,), (1,)), ((), ())), preferred_element_type=jnp.float32
    )
    return lax.psum(partial_value, "par")


def curvatures(image, smoothed):
    local_image = jnp.sum(image * image, axis=1)
    local_smooth = jnp.sum(smoothed * smoothed, axis=1)
    image_sq = lax.psum(local_image, "pix")
    smooth_sq = lax.psum(local_smooth, "par")
    return image_sq + smooth_sq


def backward_sum(rounded, green_matrix):
    return lax.psum(jnp.dot(rounded, green_matrix, preferred_element_type=jnp.float32), "pix")


def column_squares(gradient):
    return lax.psum(jnp.sum(gradient * gradient, axis=1), "par")


def on_device(green_matrix, observed):
    set_count = observed.shape[0]
    tile_cells = green_matrix.shape[1]
    residual = observed.astype(jnp.float32)
    gradient = backward_sum(observed, green_matrix)
    grad_sq = column_squares(gradient)
    direction = gradient
    solution = jnp.zeros((set_count, tile_cells), jnp.float32)
    smooth_res = jnp.zeros((set_count, tile_cells), jnp.float32)
    for sweep in range(ITERS):
        rounded = direction.astype(jnp.bfloat16)
        image = forward(rounded, green_matrix)
        smoothed = smooth(lax.optimization_barrier(rounded).astype(jnp.float32))
        step_len = (grad_sq / curvatures(image, smoothed))[:, None]
        solution = solution + step_len * direction
        residual = residual - step_len * image
        smooth_res = smooth_res - step_len * smoothed
        if sweep + 1 < ITERS:
            gradient = backward_sum(residual.astype(jnp.bfloat16), green_matrix) + smooth(
                smooth_res
            )
            fresh_sq = column_squares(gradient)
            direction = gradient + (fresh_sq / grad_sq)[:, None] * direction
            grad_sq = fresh_sq
    return (solution, residual)


MESH = pl.DeviceIdType.MESH


def to_row(column):
    count = column.shape[0]
    eye = lax.broadcasted_iota(jnp.int32, (count, LANES), 0) == lax.broadcasted_iota(
        jnp.int32, (count, LANES), 1
    )
    return jnp.sum(jnp.where(eye, jnp.broadcast_to(column, (count, LANES)), 0.0), axis=0, keepdims=True)


def to_column(row, count):
    eye = lax.broadcasted_iota(jnp.int32, (count, LANES), 0) == lax.broadcasted_iota(
        jnp.int32, (count, LANES), 1
    )
    return jnp.sum(jnp.where(eye, jnp.broadcast_to(row, (count, LANES)), 0.0), axis=1, keepdims=True)


def flipped(index, mask, count):
    value, bit = 0, 1
    while bit < count:
        digit = lax.rem(index // bit, 2)
        value = value + bit * (1 - digit if mask & bit else digit)
        bit *= 2
    return value


def far_first(count):
    masks = []
    bit = count // 2
    while bit:
        masks += range(2 * bit - 1, bit - 1, -1)
        bit //= 2
    return masks


def stencil(above, here, below):
    lane = lax.broadcasted_iota(jnp.int32, here.shape, 1)
    left = jnp.where(lane == 0, 0.0, pltpu.roll(here, 1, 1))
    right = jnp.where(lane == GRID - 1, 0.0, pltpu.roll(here, GRID - 1, 1))
    return here - 0.25 * (above + below + left + right)


def cgls_kernel(
    nz, npar,
    green_hbm, obs_hbm, x_ref, r_ref,
    obs_ref, green, green_t, imb, im, own_image, p_ext, sp, g_own, own_part, gg_ref,
    rs_send, rs_recv, ag, h_recv, halo,
    sz, sp_scalar, nz_scalar, npar_scalar,
    obs_sem, load_sem, rs_ss, rs_rs, ag_ss, ag_rs, h_ss, h_rs, halo_ss, halo_rs,
    sz_ss, sz_rs, sp_ss, sp_rs, nz_ss, nz_rs, np_ss, np_rs,
):
    me_z = lax.axis_index("pix")
    me_p = lax.axis_index("par")
    core = lax.rem(me_p, 2)
    chip = me_p // 2
    nchip = npar // 2
    partner = me_p + 1 - 2 * core
    size = obs_ref.shape[0] // GROUPS
    groups = range(GROUPS)
    width = green.shape[3]
    rows = nz * SUB * width // GRID
    own_rows = width // GRID
    edge = 2 * GRID
    z_peers = [flipped(me_z, mask, nz) for mask in far_first(nz)]
    z_from = z_peers[::-1]
    p_peers = [
        2 * lax.rem(chip + i, nchip) + c for i in range(1, nchip) for c in range(2)
    ] + [partner]
    order = [(s, c) for s in range(SUB) for c in z_peers] + [(s, me_z) for s in range(SUB)]

    def load(s, c):
        first = pl.multiple_of((c * SUB + s) * width, width)
        return pltpu.make_async_copy(
            green_hbm.at[:, pl.ds(first, width)], green.at[c, s], load_sem.at[c, s]
        )

    obs_copy = pltpu.make_async_copy(obs_hbm, obs_ref, obs_sem)
    obs_copy.start()
    for s, c in order:
        load(s, c).start()

    barrier = pltpu.get_barrier_semaphore()
    for j in range(1, nz):
        pl.semaphore_signal(barrier, inc=1, device_id={"pix": lax.rem(me_z + j, nz)}, device_id_type=MESH)
    for j in range(1, npar):
        pl.semaphore_signal(barrier, inc=1, device_id={"par": lax.rem(me_p + j, npar)}, device_id_type=MESH)

    im[...] = jnp.zeros_like(im)
    p_ext[...] = jnp.zeros_like(p_ext)
    sp[...] = jnp.zeros_like(sp)
    sz[0] = jnp.zeros_like(sz[0])
    sp_scalar[0] = jnp.zeros_like(sp_scalar[0])
    g_own[...] = jnp.zeros_like(g_own)
    gg_ref[...] = jnp.zeros_like(gg_ref)
    x_ref[...] = jnp.zeros_like(x_ref)
    obs_copy.wait()
    for g in groups:
        mine = slice(g * size, (g + 1) * size)
        imb[g] = obs_ref[mine]
        r_ref[mine] = obs_ref[mine].astype(jnp.float32)

    with jax.named_scope("barrier"):
        pl.semaphore_wait(barrier, nz + npar - 2)

    def z_copy(buf, ssem, rsem, k, g, source, target, *s):
        return pltpu.make_async_remote_copy(
            src_ref=buf.at[(k, g, source, *s)], dst_ref=buf.at[(k, g, source, *s)],
            send_sem=ssem.at[(k, g, target, *s)], recv_sem=rsem.at[(k, g, source, *s)],
            device_id={"pix": target}, device_id_type=MESH,
        )

    def to_z(buf, ssem, rsem, k, g, peer, *s):
        return z_copy(buf, ssem, rsem, k, g, me_z, peer, *s)

    def from_z(buf, ssem, rsem, k, g, peer, *s):
        return z_copy(buf, ssem, rsem, k, g, peer, peer, *s)

    def par_copy(buf, ssem, rsem, k, g, source, target):
        return pltpu.make_async_remote_copy(
            src_ref=buf.at[k, g, source], dst_ref=buf.at[k, g, source],
            send_sem=ssem.at[k, g, target], recv_sem=rsem.at[k, g, source],
            device_id={"par": target}, device_id_type=MESH,
        )

    def to_par(buf, ssem, rsem, k, g, peer):
        return par_copy(buf, ssem, rsem, k, g, me_p, peer)

    def from_par(buf, ssem, rsem, k, g, peer):
        return par_copy(buf, ssem, rsem, k, g, peer, peer)

    image_sq = (sz, sz_ss, sz_rs)
    smooth_sq = (sp_scalar, sp_ss, sp_rs)
    pix_sq = (nz_scalar, nz_ss, nz_rs)
    par_sq = (npar_scalar, np_ss, np_rs)
    gathered = (ag, ag_ss, ag_rs)
    images = (h_recv, h_ss, h_rs)

    def total_row(parts):
        value = parts[0]
        for part in parts[1:]:
            value = value + part
        return value

    def z_row(buf, k, g):
        return total_row([buf[k, g, i] for i in range(nz)])

    def par_row(buf, k, g):
        return total_row([buf[k, g, i] for i in range(npar)])

    def send_image_sq(k, g):
        image = im[g]
        row = to_row(jnp.sum(image * image, axis=1, keepdims=True))
        sz[k, g, me_z] = row
        for peer in z_peers:
            to_z(*image_sq, k, g, peer).start()

    def send_smooth_sq(k, g):
        square = jnp.zeros((size, GRID), jnp.float32)
        for i in range(rows + 2):
            line = stencil(
                p_ext[g, :, i * GRID:(i + 1) * GRID],
                p_ext[g, :, (i + 1) * GRID:(i + 2) * GRID],
                p_ext[g, :, (i + 2) * GRID:(i + 3) * GRID],
            )
            if i == 0:
                line = jnp.where(me_p == 0, 0.0, line)
            elif i == rows + 1:
                line = jnp.where(me_p == npar - 1, 0.0, line)
            else:
                square = square + line * line
            sp[g, :, i * GRID:(i + 1) * GRID] = line
        row = to_row(jnp.sum(square, axis=1, keepdims=True))
        sp_scalar[k, g, me_p] = row
        for peer in p_peers:
            to_par(*smooth_sq, k, g, peer).start()

    def wait_curvature(k, g):
        for peer in p_peers:
            from_par(*smooth_sq, k, g, peer).wait_recv()
        for peer in z_from:
            from_z(*image_sq, k, g, peer).wait_recv()

    def step_row(k, g):
        return gg_ref[g] / (z_row(sz, k, g) + par_row(sp_scalar, k, g))

    def apply_step(step, g):
        mine = slice(g * size, (g + 1) * size)
        x_ref[mine] += step * p_ext[g, :, edge:edge + rows * GRID]
        r_ref[mine] -= step * im[g]

    def finish_curvature(k, g):
        for peer in z_peers:
            to_z(*image_sq, k, g, peer).wait_send()
        for peer in p_peers:
            to_par(*smooth_sq, k, g, peer).wait_send()

    def rs_copy(k, g, target, s):
        return pltpu.make_async_remote_copy(
            src_ref=rs_send.at[k, g, target, s], dst_ref=rs_recv.at[k, g, me_z, s],
            send_sem=rs_ss.at[k, g, target, s], recv_sem=rs_rs.at[k, g, me_z, s],
            device_id={"pix": target}, device_id_type=MESH,
        )

    def rs_from(k, g, source, s):
        return pltpu.make_async_remote_copy(
            src_ref=rs_send.at[k, g, source, s], dst_ref=rs_recv.at[k, g, source, s],
            send_sem=rs_ss.at[k, g, source, s], recv_sem=rs_rs.at[k, g, source, s],
            device_id={"pix": source}, device_id_type=MESH,
        )

    up = lax.rem(me_p + 1, npar)
    down = lax.rem(me_p + npar - 1, npar)

    def halo_copies(k, g):
        return (
            pltpu.make_async_remote_copy(
                src_ref=ag.at[k, g, nz - 1, SUB - 1, :, pl.ds(width - edge, edge)],
                dst_ref=halo.at[k, g, 0],
                send_sem=halo_ss.at[k, g, 0], recv_sem=halo_rs.at[k, g, 0],
                device_id={"par": up}, device_id_type=MESH,
            ),
            pltpu.make_async_remote_copy(
                src_ref=ag.at[k, g, 0, 0, :, pl.ds(0, edge)],
                dst_ref=halo.at[k, g, 1],
                send_sem=halo_ss.at[k, g, 1], recv_sem=halo_rs.at[k, g, 1],
                device_id={"par": down}, device_id_type=MESH,
            ),
        )

    def scatter(k, g, loading=False):
        vector = imb[g]

        def backward(s, c):
            if loading:
                load(s, c).wait()
            return jnp.dot(vector, green[c, s], preferred_element_type=jnp.float32)

        with jax.named_scope("bwd%d" % g):
            turns = [(s, peer) for s in range(SUB) for peer in z_peers]
            ready = backward(*turns[0])
            for i, (s, peer) in enumerate(turns):
                value = ready
                if i + 1 < len(turns):
                    ready = backward(*turns[i + 1])
                rs_send[k, g, peer, s] = value.astype(jnp.bfloat16)
                rs_copy(k, g, peer, s).start()
        with jax.named_scope("own%d" % g):
            for s in range(SUB):
                base = (me_z * SUB + s) * own_rows
                lines = []
                for i in range(own_rows):
                    lines.append(stencil(*[
                        sp[g, :, pl.ds(pl.multiple_of((base + i + d) * GRID, GRID), GRID)]
                        for d in range(3)
                    ]))
                own_part[g, s] = backward(s, me_z) + jnp.concatenate(lines, axis=1)

    def forward(k, g, s, c):
        return jnp.dot(ag[k, g, c, s], green_t[c, s], preferred_element_type=jnp.float32)

    def gather(k, g):
        with jax.named_scope("curv%d" % g):
            @pl.when(k > 0)
            def _():
                wait_curvature(k, g)

            step = to_column(jnp.where(k == 0, -1.0, step_row(k, g)), size)
        square = jnp.zeros((size, 1), jnp.float32)
        for s in range(SUB):
            with jax.named_scope("rs%d" % g):
                for source in z_from:
                    rs_from(k, g, source, s).wait_recv()
            with jax.named_scope("upd%d" % g):
                fresh = own_part[g, s]
                for source in z_from:
                    fresh = fresh + rs_recv[k, g, source, s].astype(jnp.float32)
                gradient = g_own[g, s] - step * fresh
                g_own[g, s] = gradient
                ag[k, g, me_z, s] = gradient.astype(jnp.bfloat16)
                for peer in z_peers:
                    to_z(*gathered, k, g, peer, s).start()
                square = square + jnp.sum(gradient * gradient, axis=1, keepdims=True)
        with jax.named_scope("fown%d" % g):
            image = forward(k, g, 0, me_z)
            for s in range(1, SUB):
                image = image + forward(k, g, s, me_z)
            own_image[g] = image
        with jax.named_scope("app%d" % g):
            nz_scalar[k, g, me_z] = to_row(square)
            for peer in z_peers:
                to_z(*pix_sq, k, g, peer).start()
            apply_step(step, g)

    def forward_rest(k, g):
        image = own_image[g]
        with jax.named_scope("frest%d" % g):
            turns = [(s, source) for s in range(SUB) for source in z_from]
            for i, stop in enumerate(STOPS):
                batch = turns[STOPS[i - 1] if i else 0:stop]
                for s, source in batch:
                    from_z(*gathered, k, g, source, s).wait_recv()
                if i + 1 == len(STOPS):
                    for copy in halo_copies(k, g):
                        copy.start()
                for s, source in batch:
                    image = image + forward(k, g, s, source)
                if i == 0:
                    for source in z_from:
                        from_z(*pix_sq, k, g, source).wait_recv()
                    npar_scalar[k, g, me_p] = z_row(nz_scalar, k, g)
                    for peer in p_peers:
                        to_par(*par_sq, k, g, peer).start()
        with jax.named_scope("hsend%d" % g):
            h_recv[k, g, me_p] = image.astype(jnp.bfloat16)
            for peer in p_peers:
                to_par(*images, k, g, peer).start()

    def advance(k, g):
        with jax.named_scope("npw%d" % g):
            for peer in p_peers:
                from_par(*par_sq, k, g, peer).wait_recv()
            for copy in halo_copies(k, g):
                copy.wait_recv()
        with jax.named_scope("pupd%d" % g):
            fresh_sq = par_row(npar_scalar, k, g)
            ratio = to_column(jnp.where(k == 0, 0.0, fresh_sq / gg_ref[g]), size)
            gg_ref[g] = fresh_sq
            for c in range(nz):
                for s in range(SUB):
                    first = edge + (c * SUB + s) * width
                    where = slice(first, first + width)
                    p_ext[g, :, where] = (
                        ag[k, g, c, s].astype(jnp.float32) + ratio * p_ext[g, :, where]
                    )
            first = jnp.where(me_p == 0, 0.0, halo[k, g, 0].astype(jnp.float32))
            p_ext[g, :, :edge] = first + ratio * p_ext[g, :, :edge]
            last = jnp.where(me_p == npar - 1, 0.0, halo[k, g, 1].astype(jnp.float32))
            p_ext[g, :, edge + rows * GRID:] = last + ratio * p_ext[g, :, edge + rows * GRID:]
            send_smooth_sq(k + 1, g)
        with jax.named_scope("hw%d" % g):
            for peer in p_peers:
                from_par(*images, k, g, peer).wait_recv()
        with jax.named_scope("im%d" % g):
            part = h_recv[k, g, 0].astype(jnp.float32)
            for i in range(1, npar):
                part = part + h_recv[k, g, i].astype(jnp.float32)
            image = part + ratio * im[g]
            im[g] = image
            imb[g] = image.astype(jnp.bfloat16)
            send_image_sq(k + 1, g)

    def finish_sends(k, g):
        for peer in z_peers:
            for s in range(SUB):
                rs_copy(k, g, peer, s).wait_send()
            to_z(*pix_sq, k, g, peer).wait_send()
        for s in range(SUB):
            for peer in z_peers:
                to_z(*gathered, k, g, peer, s).wait_send()
        for copy in halo_copies(k, g):
            copy.wait_send()
        for peer in p_peers:
            to_par(*par_sq, k, g, peer).wait_send()
            to_par(*images, k, g, peer).wait_send()
        finish_curvature(k + 1, g)

    scatter(0, 0, loading=True)
    with jax.named_scope("transp"):
        for s, c in order:
            green_t[c, s] = green[c, s].T

    @pl.loop(0, ITERS)
    def _(k):
        gather(k, 0)

        @pl.when(k > 0)
        def _():
            advance(k - 1, 1)

        scatter(k, 1)

        @pl.when(k > 0)
        def _():
            finish_sends(k - 1, 1)

        forward_rest(k, 0)
        gather(k, 1)
        advance(k, 0)

        @pl.when(k + 1 < ITERS)
        def _():
            scatter(k + 1, 0)

        forward_rest(k, 1)
        finish_sends(k, 0)

    with jax.named_scope("final"):
        wait_curvature(ITERS, 0)
        apply_step(to_column(step_row(ITERS, 0), size), 0)
    advance(ITERS - 1, 1)
    with jax.named_scope("final2"):
        finish_sends(ITERS - 1, 1)
        wait_curvature(ITERS, 1)
        apply_step(to_column(step_row(ITERS, 1), size), 1)


def finish_kernel(x_ref, r_ref, x_out, r_out, x_sem, r_sem):
    copies = (
        pltpu.make_async_copy(x_ref, x_out, x_sem),
        pltpu.make_async_copy(r_ref, r_out, r_sem),
    )
    for copy in copies:
        copy.start()
    for copy in copies:
        copy.wait()


def finish(x, r):
    vmem = pl.BlockSpec(memory_space=pltpu.VMEM)
    space = pl.BlockSpec(memory_space=pl.ANY)
    return pl.pallas_call(
        finish_kernel,
        out_shape=(jax.ShapeDtypeStruct(x.shape, x.dtype), jax.ShapeDtypeStruct(r.shape, r.dtype)),
        in_specs=[vmem, vmem],
        out_specs=(space, space),
        scratch_shapes=[pltpu.SemaphoreType.DMA, pltpu.SemaphoreType.DMA],
    )(x, r)


def on_device_kernel(nz, npar, green_matrix, observed):
    sets, pixels = observed.shape
    cells = green_matrix.shape[1]
    width = cells // (nz * SUB)
    size = sets // GROUPS
    bf16, f32 = jnp.bfloat16, jnp.float32
    dma = pltpu.SemaphoreType.DMA
    n = ITERS
    vmem = pl.BlockSpec(memory_space=pltpu.VMEM)
    return pl.pallas_call(
        functools.partial(cgls_kernel, nz, npar),
        out_shape=(
            jax.ShapeDtypeStruct((sets, cells), f32),
            jax.ShapeDtypeStruct((sets, pixels), f32),
        ),
        in_specs=[pl.BlockSpec(memory_space=pl.ANY), pl.BlockSpec(memory_space=pl.ANY)],
        out_specs=(vmem, vmem),
        scratch_shapes=[
            pltpu.VMEM((sets, pixels), bf16),
            pltpu.VMEM((nz, SUB, pixels, width), bf16),
            pltpu.VMEM((nz, SUB, width, pixels), bf16),
            pltpu.VMEM((GROUPS, size, pixels), bf16),
            pltpu.VMEM((GROUPS, size, pixels), f32),
            pltpu.VMEM((GROUPS, size, pixels), f32),
            pltpu.VMEM((GROUPS, size, cells + 4 * GRID), f32),
            pltpu.VMEM((GROUPS, size, cells + 2 * GRID), f32),
            pltpu.VMEM((GROUPS, SUB, size, width), f32),
            pltpu.VMEM((GROUPS, SUB, size, width), f32),
            pltpu.VMEM((GROUPS, 1, LANES), f32),
            pltpu.VMEM((n, GROUPS, nz, SUB, size, width), bf16),
            pltpu.VMEM((n, GROUPS, nz, SUB, size, width), bf16),
            pltpu.VMEM((n, GROUPS, nz, SUB, size, width), bf16),
            pltpu.VMEM((n, GROUPS, npar, size, pixels), bf16),
            pltpu.VMEM((n, GROUPS, 2, size, 2 * GRID), bf16),
            pltpu.VMEM((n + 1, GROUPS, nz, 1, LANES), f32),
            pltpu.VMEM((n + 1, GROUPS, npar, 1, LANES), f32),
            pltpu.VMEM((n, GROUPS, nz, 1, LANES), f32),
            pltpu.VMEM((n, GROUPS, npar, 1, LANES), f32),
            dma,
            dma((nz, SUB)),
            dma((n, GROUPS, nz, SUB)), dma((n, GROUPS, nz, SUB)),
            dma((n, GROUPS, nz, SUB)), dma((n, GROUPS, nz, SUB)),
            dma((n, GROUPS, npar)), dma((n, GROUPS, npar)),
            dma((n, GROUPS, 2)), dma((n, GROUPS, 2)),
            dma((n + 1, GROUPS, nz)), dma((n + 1, GROUPS, nz)),
            dma((n + 1, GROUPS, npar)), dma((n + 1, GROUPS, npar)),
            dma((n, GROUPS, nz)), dma((n, GROUPS, nz)),
            dma((n, GROUPS, npar)), dma((n, GROUPS, npar)),
        ],
        compiler_params=pltpu.CompilerParams(
            collective_id=0, has_side_effects=True, vmem_limit_bytes=60 * 1024 * 1024
        ),
    )(green_matrix, observed)


def solution(mesh):
    nz, npar = mesh.shape["pix"], mesh.shape["par"]

    def step(green_matrix, observed):
        sets, cells = observed.shape[0], green_matrix.shape[1]
        width = cells // (nz * SUB)
        fits = cells % (nz * SUB * GRID) == 0 and width >= 2 * GRID and nz & (nz - 1) == 0
        if fits and nz > 1 and npar % 2 == 0 and sets % 32 == 0 and sets <= LANES:
            return finish(*on_device_kernel(nz, npar, green_matrix, observed))
        return on_device(green_matrix, observed)

    return jax.shard_map(
        step,
        mesh=mesh,
        in_specs=(P("pix", "par"), P("parts", "pix")),
        out_specs=(P("parts", "par"), P("parts", "pix")),
        check_vma=False,
    )
```
